256 devices in a mesh: depth: 8 (over z), col: 4 (over y), row: 8 (over x, core).
Axes of the slice: x: 4, y: 4, z: 8, core: 2. Of those that a mesh axis runs over, the one named last changes fastest.
Arguments:
- weight: bfloat16 [16384, 16384], P(('row', 'depth'), 'col')
- rhs_stack: bfloat16 [3, 16384, 4096], P(None, ('row', 'depth'), 'col')
Outputs:
- output: bfloat16 [3, 16384, 4096], P(None, ('row', 'depth'), 'col')
All inputs are finite; a program needn't handle non-finite values.
Results may differ from the reference program's by a relative error of at most 0.001.
Values are sent between devices in bfloat16 or wider.
A program may use at most 768 MiB of HBM per device.

```python
import jax
import jax.numpy as jnp
from jax import lax

N = 16384
RHS_COLS = 4096


def setup_inputs(seed: int = 0) -> dict:
    base_key = jax.random.key(seed)
    key_w, key_x = jax.random.split(base_key)
    weight = jax.random.normal(key_w, (N, N), jnp.float32) * (N ** -0.5) + 2.0 / N
    rhs_stack = jax.random.normal(key_x, (3, N, RHS_COLS), jnp.float32) + 0.5
    return {"weight": weight.astype(jnp.bfloat16), "rhs_stack": rhs_stack.astype(jnp.bfloat16)}


def reference(weight, rhs_stack):
    def one_product(rhs_block):
        return jnp.dot(weight, rhs_block, preferred_element_type=jnp.float32).astype(jnp.bfloat16)
    return lax.map(one_product, rhs_stack)
```

```python
import heapq

import jax
import jax.numpy as jnp
from jax import lax
from jax.experimental import pallas as pl
from jax.experimental.pallas import tpu as pltpu
from jax.sharding import PartitionSpec as P

MESH = pl.DeviceIdType.MESH
XS = 4
YS = 4
RHS = 3

A_UNIT_US = 11.3
X_UNIT_US = 8.5
A2A_UNIT_US = 2.9
D2D_UNIT_US = 4.0
HOP_US = 3.0
BLOCK_US = 9.0
PART_US = 2.6


def a_sends(unit):
    dx, dy, half, piece = unit
    major, minor = (dx, dy) if half == 0 else (dy, dx)
    fwd, back = ("x+", "x-") if half == 0 else ("y+", "y-")
    fwd2, back2 = ("y+", "y-") if half == 0 else ("x+", "x-")

    def named(new_major, new_minor):
        return (new_major, new_minor, half, piece) if half == 0 else (new_minor, new_major, half, piece)

    out = []
    if minor == 0:
        if major == 0:
            out += [(fwd, named(1, 0)), (back, named(3, 0))]
        elif major == 1 and piece == 0:
            out += [(fwd, named(2, 0))]
        elif major == 3 and piece == 1:
            out += [(back, named(2, 0))]
        out += [(fwd2, named(major, 1)), (back2, named(major, 3))]
    elif minor == 1 and piece == 0:
        out += [(fwd2, named(major, 2))]
    elif minor == 3 and piece == 1:
        out += [(back2, named(major, 2))]
    return out


def x_sends(unit, depth_size):
    dx, dz = unit
    mid = depth_size // 2
    out = []
    if dz < mid and (dz + 1 < mid or dx in (0, 1)):
        out.append(("z+", (dx, dz + 1)))
    back = (depth_size - dz) % depth_size
    if (dz == 0 or dz > mid) and (back + 1 < mid or dx not in (0, 1)):
        out.append(("z-", (dx, (dz - 1) % depth_size)))
    return out


def plan(depth_size):
    steps = []
    link_free = {}
    heap = []
    count = 0

    def send(link, name, now, cost):
        nonlocal count
        begin = max(now, link_free.get(link, 0.0))
        link_free[link] = begin + cost
        heapq.heappush(heap, (begin + cost + HOP_US, count, name))
        count += 1

    def handle(name, now):
        kind, unit = name
        steps.append(("have", name))
        if kind == "A":
            for link, there in a_sends(unit):
                send(link, ("A", there), now, A_UNIT_US)
        elif kind == "X":
            for link, there in x_sends(unit, depth_size):
                send(link, ("X", there), now, X_UNIT_US)

    for dx, link in ((1, "x+"), (3, "x-"), (2, "x+")):
        send(link, ("X", (dx, 0)), 0.0, 3 * A2A_UNIT_US)
    handle(("X", (0, 0)), 0.0)
    for half, piece in ((0, 0), (1, 0), (0, 1), (1, 1)):
        handle(("A", (0, 0, half, piece)), 0.0)

    done = set([("X", (0, 0))]) | set(("A", (0, 0, h, p)) for h in range(2) for p in range(2))
    x_all = set(("X", (dx, dz)) for dx in range(XS) for dz in range(depth_size))
    shared = set()

    def a_need(dxs, dy):
        return set(("A", (dx, dy, h, p)) for dx in dxs for h in range(2) for p in range(2))

    blocks = [(("mm", dy, None), a_need(range(XS), dy), BLOCK_US) for dy in (0, 1, 3)]
    blocks += [(("mm", 2, dx), a_need((dx,), 2), PART_US) for dx in (2, 1, 3, 0)]
    now = 0.0
    have_peer = False
    while heap or blocks:
        while heap and heap[0][0] <= now:
            _, _, name = heapq.heappop(heap)
            done.add(name)
            handle(name, now)
        for dz in range(depth_size):
            if dz not in shared and all(("X", (dx, dz)) in done for dx in range(XS)):
                shared.add(dz)
                steps.append(("share", dz))
                peer_at = now + D2D_UNIT_US + HOP_US
        ready = None
        if x_all <= done and now >= peer_at:
            if not have_peer:
                have_peer = True
                steps.append(("peer",))
            early = [b for b in blocks if b[0][2] is None]
            for block in (early or blocks):
                if block[1] <= done:
                    ready = block
                    break
        if ready is not None:
            blocks.remove(ready)
            steps.append(ready[0])
            now += ready[2]
        elif heap:
            now = max(now, heap[0][0])
        else:
            now = max(now, peer_at)
    return steps, now


def solution(mesh):
    depth_size = mesh.shape["depth"]
    steps, _ = plan(depth_size)

    def kernel(w_ref, x_ref, o_ref, a_all, x_all, acc, y_buf,
               a_ssem, a_rsem, x_ssem, x_rsem, d_ssem, d_rsem, t_ssem, t_rsem, y_ssem, y_rsem, l_sem):
        layer = lax.axis_index("depth")
        col = lax.axis_index("col")
        row = lax.axis_index("row")
        core = lax.rem(row, 2)
        xpos = row // 2
        rows, kcols = w_ref.shape
        unit = rows // 4
        sub = x_ref.shape[2] // XS

        def mod(value, size):
            return lax.rem(value + size, size)

        def row_peer(hops):
            return {"row": lax.rem(row + 2 * hops, 2 * XS)}

        sibling = {"row": row + 1 - 2 * core}
        links = {
            "x+": row_peer(1),
            "x-": row_peer(3),
            "y+": {"col": lax.rem(col + 1, YS)},
            "y-": {"col": lax.rem(col + YS - 1, YS)},
            "z+": {"depth": lax.rem(layer + 1, depth_size)},
            "z-": {"depth": lax.rem(layer + depth_size - 1, depth_size)},
        }

        barrier = pltpu.get_barrier_semaphore()
        partners = list(links.values()) + [row_peer(2), sibling]
        for partner in partners:
            pl.semaphore_signal(barrier, inc=1, device_id=partner, device_id_type=MESH)
        pl.semaphore_wait(barrier, len(partners))

        sent = []

        def a_index(name):
            dx, dy, half, piece = name
            return ((dx * 4 + dy) * 2 + half) * 2 + piece

        def a_slot(name):
            dx, dy, half, piece = name
            start = mod(xpos - dx, XS) * rows + (half * 2 + piece) * unit
            return a_all.at[mod(col - dy, YS), pl.ds(pl.multiple_of(start, unit), unit), :]

        def x_index(name):
            return name[1] * 4 + name[0]

        def x_rows(core_idx, dz):
            start = (core_idx * depth_size + mod(layer - dz, depth_size)) * rows
            return pl.ds(pl.multiple_of(start, rows), rows)

        def x_slot(name):
            return x_all.at[mod(xpos - name[0], XS), x_rows(core, name[1]), :]

        def remote(src, dst, ssem, rsem, device):
            copy = pltpu.make_async_remote_copy(src_ref=src, dst_ref=dst, send_sem=ssem, recv_sem=rsem, device_id=device, device_id_type=MESH)
            copy.start()
            sent.append(copy)

        def landed(slot, rsem):
            pltpu.make_async_remote_copy(src_ref=slot, dst_ref=slot, send_sem=l_sem.at[0], recv_sem=rsem, device_id=sibling, device_id_type=MESH).wait_recv()

        def x_part(hops, r):
            start = mod(xpos + hops, XS) * sub
            return x_ref.at[r, :, pl.ds(pl.multiple_of(start, sub), sub)]

        def x_dest(dx, r):
            return x_all.at[mod(xpos - dx, XS), x_rows(core, 0), pl.ds(r * sub, sub)]

        own_x = [pltpu.make_async_copy(x_part(0, r), x_dest(0, r), l_sem.at[1 + r]) for r in range(RHS)]
        for copy in own_x:
            copy.start()
        for hops in (1, 3, 2):
            for r in range(RHS):
                sem = hops * RHS + r
                remote(x_part(hops, r), x_dest(0, r), t_ssem.at[sem], t_rsem.at[sem], row_peer(hops))
        own_a = pltpu.make_async_copy(w_ref, a_all.at[col, pl.ds(pl.multiple_of(xpos * rows, rows), rows), :], l_sem.at[1 + RHS])
        own_a.start()
        acc[...] = jnp.zeros_like(acc)

        def matmul(dy, dx):
            chunk = mod(col - dy, YS)
            if dx is None:
                row0, nrows = 0, XS * rows
            else:
                row0, nrows = pl.multiple_of(mod(xpos - dx, XS) * rows, rows), rows
            kstep = min(1024, kcols)

            def body(idx, carry):
                r = idx // (kcols // kstep)
                k0 = pl.multiple_of(lax.rem(idx, kcols // kstep) * kstep, kstep)
                n0 = pl.multiple_of(r * sub, sub)
                lhs = a_all[chunk, pl.ds(row0, nrows), pl.ds(k0, kstep)]
                rhs = x_all[chunk, pl.ds(k0, kstep), pl.ds(n0, sub)]
                acc[pl.ds(row0, nrows), pl.ds(n0, sub)] += jnp.dot(lhs, rhs, preferred_element_type=jnp.float32)
                return carry

            lax.fori_loop(0, RHS * (kcols // kstep), body, 0)

        local = []

        def finish(dx):
            row0 = pl.multiple_of(mod(xpos - dx, XS) * rows, rows)
            for r in range(RHS):
                y_buf[dx, r] = acc[pl.ds(row0, rows), pl.ds(r * sub, sub)].astype(y_buf.dtype)
            dst = o_ref.at[:, :, pl.ds(pl.multiple_of(xpos * sub, sub), sub)]
            if dx == 0:
                copy = pltpu.make_async_copy(y_buf.at[0], dst, l_sem.at[2 + RHS])
                copy.start()
                local.append(copy)
            else:
                remote(y_buf.at[dx], dst, y_ssem.at[dx], y_rsem.at[dx], row_peer(XS - dx))

        own_waited = False
        for step in steps:
            if step[0] == "have":
                kind, name = step[1]
                if kind == "A":
                    if name[:2] != (0, 0):
                        landed(a_slot(name), a_rsem.at[a_index(name)])
                    for link, there in a_sends(name):
                        if name[:2] == (0, 0):
                            src = w_ref.at[pl.ds((name[2] * 2 + name[3]) * unit, unit), :]
                        else:
                            src = a_slot(name)
                        idx = a_index(there)
                        remote(src, a_slot(name), a_ssem.at[idx], a_rsem.at[idx], links[link])
                else:
                    if name == (0, 0):
                        for copy in own_x:
                            copy.wait()
                    elif name[1] == 0:
                        for r in range(RHS):
                            landed(x_dest(name[0], r), t_rsem.at[name[0] * RHS + r])
                    else:
                        landed(x_slot(name), x_rsem.at[x_index(name)])
                    for link, there in x_sends(name, depth_size):
                        idx = x_index(there)
                        remote(x_slot(name), x_slot(name), x_ssem.at[idx], x_rsem.at[idx], links[link])
            elif step[0] == "share":
                slot = x_all.at[:, x_rows(core, step[1]), :]
                remote(slot, slot, d_ssem.at[step[1]], d_rsem.at[step[1]], sibling)
            elif step[0] == "peer":
                for dz in range(depth_size):
                    landed(x_all.at[:, x_rows(1 - core, dz), :], d_rsem.at[dz])
            else:
                if not own_waited:
                    own_waited = True
                    own_a.wait()
                matmul(step[1], step[2])
                if step[2] is not None:
                    finish(step[2])

        for dx in range(1, XS):
            slot = o_ref.at[:, :, pl.ds(pl.multiple_of(mod(xpos + dx, XS) * sub, sub), sub)]
            landed(slot, y_rsem.at[dx])
        for copy in local:
            copy.wait()
        for copy in sent:
            copy.wait_send()

    def local_product(w_local, x_local):
        rows, kcols = w_local.shape
        sub = x_local.shape[2] // XS
        dma = pltpu.SemaphoreType.DMA
        return pl.pallas_call(
            kernel,
            out_shape=jax.ShapeDtypeStruct(x_local.shape, jnp.bfloat16),
            in_specs=[pl.BlockSpec(memory_space=pl.ANY)] * 2,
            out_specs=pl.BlockSpec(memory_space=pl.ANY),
            scratch_shapes=[
                pltpu.VMEM((YS, XS * rows, kcols), jnp.bfloat16),
                pltpu.VMEM((XS, kcols, RHS * sub), jnp.bfloat16),
                pltpu.VMEM((XS * rows, RHS * sub), jnp.float32),
                pltpu.VMEM((XS, RHS, rows, sub), jnp.bfloat16),
                dma((64,)), dma((64,)),
                dma((4 * depth_size,)), dma((4 * depth_size,)),
                dma((depth_size,)), dma((depth_size,)),
                dma((XS * RHS,)), dma((XS * RHS,)),
                dma((XS,)), dma((XS,)),
                dma((8,)),
            ],
            compiler_params=pltpu.CompilerParams(collective_id=0, has_side_effects=True, vmem_limit_bytes=67043328),
            cost_estimate=pl.CostEstimate(flops=2 * XS * rows * YS * kcols * RHS * sub, bytes_accessed=0, transcendentals=0),
            name="gather_matmul",
        )(w_local, x_local)

    return jax.shard_map(local_product, mesh=mesh, in_specs=(P(("row", "depth"), "col"), P(None, ("row", "depth"), "col")), out_specs=P(None, ("row", "depth"), "col"), check_vma=False)
```

```python
import heapq

import jax
import jax.numpy as jnp
from jax import lax
from jax.experimental import pallas as pl
from jax.experimental.pallas import tpu as pltpu
from jax.sharding import PartitionSpec as P

MESH = pl.DeviceIdType.MESH
XS = 4
YS = 4
RHS = 3
CHUNKS = 6
POS = {0: 0, 1: 1, 3: 2, 2: 3}
GROUPS = ((0,), (1, 3), (2,))

A_UNIT_US = 11.3
X_UNIT_US = 5.65
T_UNIT_US = 3.0
D2D_US = 1.5
XCH_US = 2.9
HOP_US = 2.5
LOOKAHEAD_US = 9.0
BLOCK_US = 1.5


def a_sends(name):
    _, dx, dp, half, piece = name
    out = []

    def along_x():
        if dx == 0:
            out.append(("x+", ("A", 1, dp, half, piece)))
            out.append(("x-", ("A", 3, dp, half, piece)))
        elif dx == 1 and piece == 0:
            out.append(("x+", ("A", 2, dp, half, piece)))
        elif dx == 3 and piece == 1:
            out.append(("x-", ("A", 2, dp, half, piece)))

    if half == 0:
        if dp == 0:
            along_x()
            out.append(("ya", ("A", dx, 1, half, piece)))
    else:
        if dp == 0 and dx == 0:
            out.append(("ya", ("A", 0, 1, half, piece)))
        along_x()
    return out


def x_sends(name, depth_size):
    _, n, dz = name
    mid = depth_size // 2
    out = []
    if dz < mid:
        out.append(("z+", ("X", n, dz + 1) if dz + 1 < mid else ("XH", n, 0)))
    back = (depth_size - dz) % depth_size
    if back < mid:
        out.append(("z-", ("X", n, (dz - 1) % depth_size) if back + 1 < mid else ("XH", n, 1)))
    return out


def plan(depth_size):
    mid = depth_size // 2
    steps, heap, pools, link_free = [], [], {}, {}
    have = set()
    count = 0

    def arrive(when, name):
        nonlocal count
        heapq.heappush(heap, (when, count, name))
        count += 1

    def cost(name):
        if name[0] == "A":
            return A_UNIT_US
        return X_UNIT_US if name[0] == "X" else X_UNIT_US / 2

    def priority(name):
        if name[0] == "A":
            return (GROUPS.index(next(g for g in GROUPS if name[1] in g)), name[4])
        return (name[1],)

    def pump(now, ahead):
        for link, pool in pools.items():
            while pool and link_free.get(link, 0.0) < now + ahead:
                pool.sort()
                _, _, src, dst = pool.pop(0)
                begin = max(now, link_free.get(link, 0.0))
                link_free[link] = begin + cost(dst)
                arrive(begin + cost(dst) + HOP_US, dst)
                steps.append(("send", link, src, dst))

    def offer(link, src, dst):
        nonlocal count
        pools.setdefault(link, []).append((priority(dst), count, src, dst))
        count += 1

    def got(name, now):
        have.add(name)
        if name[0] == "A":
            for link, there in a_sends(name):
                offer(link, name, there)
        elif name[0] in ("T", "X"):
            unit = ("X", name[1], 0) if name[0] == "T" else name
            for link, there in x_sends(unit, depth_size):
                offer(link, unit, there)
            share(name[1], unit[2], now)
        elif name[0] == "XH" and ("XH", name[1], 1 - name[2]) in have:
            share(name[1], mid, now)

    def share(n, dz, now):
        steps.append(("share", n, dz))
        arrive(now + D2D_US + HOP_US, ("P", n, dz))

    now = 0.0
    for n in range(CHUNKS):
        arrive(HOP_US + 2.0 + (n + 1) * T_UNIT_US, ("T", n))
    steps.append(("a2a", 0))
    steps.append(("a2a", 1))
    for half, piece in ((0, 0), (1, 0), (0, 1), (1, 1)):
        got(("A", 0, 0, half, piece), now)
    pump(now, LOOKAHEAD_US)
    for n in range(2, CHUNKS):
        steps.append(("a2a", n))

    def needs(g, n):
        out = set(("A", dx, dp, half, piece) for dx in GROUPS[g] for dp in range(2) for half in range(2) for piece in range(2))
        out |= set(("P", n, dz) for dz in range(depth_size))
        out |= set(("X", n, dz) for dz in range(1, depth_size) if dz != mid) | {("T", n), ("XH", n, 0), ("XH", n, 1)}
        return out

    blocks = [(g, n) for n in range(CHUNKS) for g in range(len(GROUPS))]
    need = {b: needs(*b) for b in blocks}
    unsent = []
    while heap or blocks or unsent:
        while heap and heap[0][0] <= now:
            _, _, name = heapq.heappop(heap)
            if name[0] == "E":
                steps.append(("fin", name[1], name[2]))
                continue
            if name[0] != "P":
                steps.append(("wait", name))
            got(name, now)
            pump(now, LOOKAHEAD_US)
        ready = next((b for b in blocks if need[b] <= have), None)
        if ready is not None:
            blocks.remove(ready)
            g, n = ready
            spent = BLOCK_US * len(GROUPS[g])
            pump(now, LOOKAHEAD_US + spent)
            steps.append(("mm", g, n))
            now += spent
            steps.append(("xch", g, n))
            begin = max(now, link_free.get("yp", 0.0))
            link_free["yp"] = begin + XCH_US * len(GROUPS[g])
            arrive(link_free["yp"] + HOP_US, ("E", g, n))
        elif heap:
            now = max(now, heap[0][0])
        pump(now, LOOKAHEAD_US)
        if not heap and not blocks:
            break
    assert not blocks and not any(pools.values())
    return steps, now


def solution(mesh):
    depth_size = mesh.shape["depth"]
    mid = depth_size // 2
    steps, _ = plan(depth_size)

    def kernel(w_ref, x_ref, o_ref, a_all, x_all, acc, peer_acc, y_buf,
               a_ssem, a_rsem, x_ssem, x_rsem, d_ssem, d_rsem, t_ssem, t_rsem, e_ssem, e_rsem, y_ssem, y_rsem, l_sem):
        layer = lax.axis_index("depth")
        col = lax.axis_index("col")
        row = lax.axis_index("row")
        core = lax.rem(row, 2)
        xpos = row // 2
        rows, kcols = w_ref.shape
        unit = rows // 4
        hrows = rows // 2
        sub = x_ref.shape[2] // 4

        xh = xpos // 2
        yh = col // 2
        q = lax.rem((col + 1) // 2, 2)

        def col_of(high):
            return q + high * (3 - 2 * q)

        def at(x, y):
            return {"row": 2 * x + core, "col": y}

        src_col = col_of(1 - xh)
        own_out = lax.rem(xh + yh, 2)
        sources = [at(2 * yh + s, src_col) for s in range(2)]
        dests = [at(2 * (1 - yh) + b, col_of(xh)) for b in range(2)]
        makers = [(b, hi, at(2 * (1 - yh) + b, col_of(hi))) for b in range(2) for hi in range(2)]
        sibling = {"row": row + 1 - 2 * core}
        links = {
            "x+": {"row": lax.rem(row + 2, 2 * XS)},
            "x-": {"row": lax.rem(row + 6, 2 * XS)},
            "ya": {"col": col + 1 - 2 * lax.rem(col, 2)},
            "yp": {"col": 3 - col},
            "z+": {"depth": lax.rem(layer + 1, depth_size)},
            "z-": {"depth": lax.rem(layer + depth_size - 1, depth_size)},
        }

        def is_self(b, hi):
            same = (1 - lax.rem(xpos + b, 2)) * (1 - lax.rem(yh + hi, 2))
            return own_out * same

        barrier = pltpu.get_barrier_semaphore()
        partners = list(links.values()) + [sibling] + sources + dests
        for partner in partners:
            pl.semaphore_signal(barrier, inc=1, device_id=partner, device_id_type=MESH)
        for b, hi, maker in makers:
            @pl.when(is_self(b, hi) == 0)
            def _():
                pl.semaphore_signal(barrier, inc=1, device_id=maker, device_id_type=MESH)
        pl.semaphore_wait(barrier, len(partners) + 4 - own_out)

        sent = []

        def a_index(name):
            return ((name[1] * 2 + name[2]) * 2 + name[3]) * 2 + name[4]

        def a_slot(name):
            _, dx, dp, half, piece = name
            return a_all.at[dp, pl.ds(POS[dx] * rows + half * hrows + piece * unit, unit), :]

        def x_index(name):
            return name[1] * (depth_size + 1) + (depth_size if name == ("XH", name[1], 1) else mid if name[0] == "XH" else name[2])

        def x_rows(core_idx, dz):
            start = (core_idx * depth_size + lax.rem(layer + depth_size - dz, depth_size)) * rows
            return pl.ds(pl.multiple_of(start, rows), rows)

        def x_slot(name):
            if name[0] == "XH":
                return x_all.at[name[1], name[2], x_rows(core, mid), :]
            return x_all.at[name[1], :, x_rows(core, name[2]), :]

        def x_out(src, there):
            if there[0] == "XH":
                return x_all.at[there[1], there[2], x_rows(core, src[2]), :]
            return x_slot(src)

        def remote(src, dst, ssem, rsem, device):
            copy = pltpu.make_async_remote_copy(src_ref=src, dst_ref=dst, send_sem=ssem, recv_sem=rsem, device_id=device, device_id_type=MESH)
            copy.start()
            sent.append(copy)

        def landed(slot, rsem):
            pltpu.make_async_remote_copy(src_ref=slot, dst_ref=slot, send_sem=l_sem.at[0], recv_sem=rsem, device_id=sibling, device_id_type=MESH).wait_recv()

        def columns(n, half):
            return pl.ds(pl.multiple_of((half * 2 + n % 2) * sub, sub), sub)

        own_a = pltpu.make_async_copy(w_ref, a_all.at[0, pl.ds(0, rows), :], l_sem.at[1])

        def exchange_x(n):
            s = lax.rem(xpos + col_of(xh), 2)
            for b in range(2):
                src = x_ref.at[n // 2, :, columns(n, b)]
                remote(src, x_all.at[n, s, x_rows(core, 0), :], t_ssem.at[n * 2 + b], t_rsem.at[n * 2 + s], dests[b])

        def matmul(g, n):
            first, count = POS[GROUPS[g][0]], len(GROUPS[g])
            kstep = min(2048, kcols)
            per = kcols // kstep

            def body(idx, carry):
                dp = idx // per
                k0 = pl.multiple_of(lax.rem(idx, per) * kstep, kstep)
                lhs = a_all[dp, pl.ds(first * rows, count * rows), pl.ds(k0, kstep)]
                rhs = x_all[n, dp, pl.ds(k0, kstep), :]
                part = jnp.dot(lhs, rhs, preferred_element_type=jnp.float32)
                acc[n, pl.ds(first, count)] += part.reshape(count, rows, sub)
                return carry

            lax.fori_loop(0, 2 * per, body, 0)

        def span(g):
            return pl.ds(POS[GROUPS[g][0]], len(GROUPS[g]))

        def exchange_acc(g, n):
            src = acc.at[n, span(g), pl.ds(pl.multiple_of((1 - yh) * hrows, hrows), hrows), :]
            idx = n * len(GROUPS) + g
            remote(src, peer_acc.at[n, span(g)], e_ssem.at[idx], e_rsem.at[idx], links["yp"])

        def out_slot(n, half, hi):
            return o_ref.at[n // 2, pl.ds(pl.multiple_of(hi * hrows, hrows), hrows), columns(n, half)]

        def y_sem(n, half, hi):
            return n * 4 + half * 2 + hi

        def finish(g, n):
            idx = n * len(GROUPS) + g
            landed(peer_acc.at[n, span(g)], e_rsem.at[idx])
            mine = pl.ds(pl.multiple_of(yh * hrows, hrows), hrows)
            y_buf[n, span(g)] = (acc[n, span(g), mine, :] + peer_acc[n, span(g)]).astype(y_buf.dtype)
            half = lax.rem(xpos, 2)
            for dx in GROUPS[g]:
                src = y_buf.at[n, POS[dx]]
                dst = out_slot(n, half, yh)
                ssem = y_ssem.at[n * 4 + dx]
                target = at(lax.rem(xpos + XS - dx, XS), src_col)

                def go():
                    pltpu.make_async_remote_copy(src_ref=src, dst_ref=dst, send_sem=ssem, recv_sem=y_rsem.at[y_sem(n, half, yh)], device_id=target, device_id_type=MESH).start()

                if dx == 0:
                    pl.when(own_out == 1)(lambda: pltpu.make_async_copy(src, dst, ssem).start())
                    pl.when(own_out == 0)(go)
                else:
                    go()

        waited = set()
        for step in steps:
            if step[0] == "a2a":
                exchange_x(step[1])
                if step[1] == CHUNKS - 1:
                    own_a.start()
                    acc[...] = jnp.zeros_like(acc)
            elif step[0] == "send":
                _, link, src, dst = step
                if dst[0] == "A":
                    if src[1:3] == (0, 0):
                        ref = w_ref.at[pl.ds(src[3] * hrows + src[4] * unit, unit), :]
                    else:
                        ref = a_slot(src)
                    idx = a_index(dst)
                    remote(ref, a_slot(dst), a_ssem.at[idx], a_rsem.at[idx], links[link])
                else:
                    idx = x_index(dst)
                    ref = x_out(src, dst)
                    remote(ref, ref, x_ssem.at[idx], x_rsem.at[idx], links[link])
            elif step[0] == "wait":
                name = step[1]
                if name[0] == "A":
                    landed(a_slot(name), a_rsem.at[a_index(name)])
                elif name[0] == "T":
                    for s in range(2):
                        landed(x_all.at[name[1], s, x_rows(core, 0), :], t_rsem.at[name[1] * 2 + s])
                else:
                    landed(x_slot(name), x_rsem.at[x_index(name)])
            elif step[0] == "share":
                _, n, dz = step
                slot = x_all.at[n, :, x_rows(core, dz), :]
                remote(slot, slot, d_ssem.at[n * depth_size + dz], d_rsem.at[n * depth_size + dz], sibling)
            elif step[0] == "mm":
                _, g, n = step
                if "a" not in waited:
                    waited.add("a")
                    own_a.wait()
                if n not in waited:
                    waited.add(n)
                    for dz in range(depth_size):
                        landed(x_all.at[n, :, x_rows(1 - core, dz), :], d_rsem.at[n * depth_size + dz])
                matmul(g, n)
            elif step[0] == "xch":
                exchange_acc(step[1], step[2])
            else:
                finish(step[1], step[2])

        for n in range(CHUNKS):
            for b in range(2):
                for hi in range(2):
                    slot = out_slot(n, b, hi)
                    sem = y_rsem.at[y_sem(n, b, hi)]
                    pl.when(is_self(b, hi) == 0)(lambda: landed(slot, sem))
            for dx in range(XS):
                src = y_buf.at[n, POS[dx]]
                pltpu.make_async_copy(src, src, y_ssem.at[n * 4 + dx]).wait()
        for copy in sent:
            copy.wait_send()

    def local_product(w_local, x_local):
        rows, kcols = w_local.shape
        sub = x_local.shape[2] // 4
        dma = pltpu.SemaphoreType.DMA

        def sems(size):
            return [dma((size,)), dma((size,))]

        return pl.pallas_call(
            kernel,
            out_shape=jax.ShapeDtypeStruct(x_local.shape, jnp.bfloat16),
            in_specs=[pl.BlockSpec(memory_space=pl.ANY)] * 2,
            out_specs=pl.BlockSpec(memory_space=pl.ANY),
            scratch_shapes=[
                pltpu.VMEM((2, XS * rows, kcols), jnp.bfloat16),
                pltpu.VMEM((CHUNKS, 2, kcols, sub), jnp.bfloat16),
                pltpu.VMEM((CHUNKS, XS, rows, sub), jnp.float32),
                pltpu.VMEM((CHUNKS, XS, rows // 2, sub), jnp.float32),
                pltpu.VMEM((CHUNKS, XS, rows // 2, sub), jnp.bfloat16),
                *sems(32), *sems(CHUNKS * (depth_size + 1)), *sems(CHUNKS * depth_size),
                *sems(CHUNKS * 2), *sems(CHUNKS * len(GROUPS)), *sems(CHUNKS * 4), dma((2,)),
            ],
            compiler_params=pltpu.CompilerParams(collective_id=0, has_side_effects=True, vmem_limit_bytes=67043328),
            cost_estimate=pl.CostEstimate(flops=2 * XS * rows * 2 * kcols * CHUNKS * sub, bytes_accessed=0, transcendentals=0),
            name="gather_matmul",
        )(w_local, x_local)

    return jax.shard_map(local_product, mesh=mesh, in_specs=(P(("row", "depth"), "col"), P(None, ("row", "depth"), "col")), out_specs=P(None, ("row", "depth"), "col"), check_vma=False)
```

```python
import heapq

import jax
import jax.numpy as jnp
from jax import lax
from jax.experimental import pallas as pl
from jax.experimental.pallas import tpu as pltpu
from jax.sharding import PartitionSpec as P

MESH = pl.DeviceIdType.MESH
XS = 4
YS = 4
RHS = 3
CHUNKS = 2 * RHS
ORDER = (0, 1, 2, 3, 4, 5)
POS = {0: 0, 1: 1, 3: 2, 2: 3}
READY = ((0,), (1,), (3,), (2,))

A_UNIT_US = 11.3
X_UNIT_US = 5.65
T_AT_US = (16.0, 27.0, 38.0, 8.0, 30.0, 60.0)
D2D_US = 1.5
XCH_US = 5.65
HOP_US = 2.5
LOOKAHEAD_US = 2.0
BLOCK_US = 1.4
FIN_US = 0.3


def a_sends(name):
    _, dx, dp, half, piece = name
    out = []

    def along_x():
        if dx == 0:
            out.append(("x+", ("A", 1, dp, half, piece)))
            out.append(("x-", ("A", 3, dp, half, piece)))
        elif dx == 1 and piece == 0:
            out.append(("x+", ("A", 2, dp, half, piece)))
        elif dx == 3 and piece == 1:
            out.append(("x-", ("A", 2, dp, half, piece)))

    if half == 0:
        if dp == 0:
            along_x()
            out.append(("ya", ("A", dx, 1, half, piece)))
    else:
        if dp == 0 and dx == 0:
            out.append(("ya", ("A", 0, 1, half, piece)))
        along_x()
    return out


def x_sends(name, depth_size):
    _, n, dz = name
    mid = depth_size // 2
    out = []
    if dz < mid:
        out.append(("z+", ("X", n, dz + 1) if dz + 1 < mid else ("XH", n, 0)))
    back = (depth_size - dz) % depth_size
    if back < mid:
        out.append(("z-", ("X", n, (dz - 1) % depth_size) if back + 1 < mid else ("XH", n, 1)))
    return out


def plan(depth_size):
    mid = depth_size // 2
    steps, heap, pools, link_free = [], [], {}, {}
    have = set()
    count = 0

    def arrive(when, name):
        nonlocal count
        heapq.heappush(heap, (when, count, name))
        count += 1

    def cost(name):
        if name[0] == "A":
            return A_UNIT_US
        return X_UNIT_US if name[0] == "X" else X_UNIT_US / 2

    def priority(name):
        if name[0] == "A":
            return (next(i for i, g in enumerate(READY) if name[1] in g), name[4])
        return (ORDER.index(name[1]),)

    def pump(now, ahead):
        for link, pool in pools.items():
            while pool and link_free.get(link, 0.0) < now + ahead:
                pool.sort()
                _, _, src, dst = pool.pop(0)
                begin = max(now, link_free.get(link, 0.0))
                link_free[link] = begin + cost(dst)
                arrive(begin + cost(dst) + HOP_US, dst)
                steps.append(("send", link, src, dst))

    def offer(link, src, dst):
        nonlocal count
        pools.setdefault(link, []).append((priority(dst), count, src, dst))
        count += 1

    def got(name, now):
        have.add(name)
        if name[0] == "A":
            for link, there in a_sends(name):
                offer(link, name, there)
        elif name[0] in ("T", "X"):
            unit = ("X", name[1], 0) if name[0] == "T" else name
            for link, there in x_sends(unit, depth_size):
                offer(link, unit, there)
            share(name[1], unit[2], now)
        elif name[0] == "XH" and ("XH", name[1], 1 - name[2]) in have:
            share(name[1], mid, now)

    def share(n, dz, now):
        steps.append(("share", n, dz))
        arrive(now + D2D_US + HOP_US, ("P", n, dz))

    now = 0.0
    for n in range(CHUNKS):
        arrive(T_AT_US[n], ("T", n))
    steps.append(("a2a", 0))
    for half, piece in ((0, 0), (1, 0), (0, 1), (1, 1)):
        got(("A", 0, 0, half, piece), now)
    pump(now, LOOKAHEAD_US)
    for r in range(1, RHS):
        steps.append(("a2a", r))

    def a_need(pos):
        return set(("A", dx, dp, half, piece) for dx in POS if POS[dx] == pos for dp in range(2) for half in range(2) for piece in range(2))

    def x_need(n):
        out = set(("P", n, dz) for dz in range(depth_size))
        return out | set(("X", n, dz) for dz in range(1, depth_size) if dz != mid) | {("T", n), ("XH", n, 0), ("XH", n, 1)}

    left = [(n, pos) for n in ORDER for pos in range(XS)]
    made, arrived, finished = set(), set(), set()

    def next_block():
        for n in ORDER:
            run = [pos for pos in range(XS) if (n, pos) in left and a_need(pos) <= have]
            if run and x_need(n) <= have:
                stop = run[0] + 1
                while stop in run:
                    stop += 1
                return n, run[0], stop
        return None

    def finish_ready():
        for r in range(RHS):
            for pos in range(XS):
                if (r, pos) in arrived and (RHS + r, pos) in made and (r, pos) not in finished:
                    finished.add((r, pos))
                    steps.append(("fin", r, pos))

    while heap or left:
        while heap and heap[0][0] <= now:
            _, _, name = heapq.heappop(heap)
            if name[0] == "E":
                _, n, lo, hi = name
                steps.append(("peer", n, lo, hi))
                arrived |= set((n, pos) for pos in range(lo, hi))
                finish_ready()
                continue
            if name[0] != "P":
                steps.append(("wait", name))
            got(name, now)
            pump(now, LOOKAHEAD_US)
        block = next_block()
        if block is not None:
            n, lo, hi = block
            left = [b for b in left if b[0] != n or not lo <= b[1] < hi]
            spent = BLOCK_US * (hi - lo)
            pump(now, LOOKAHEAD_US + spent)
            steps.append(("mm", n, lo, hi))
            now += spent
            made |= set((n, pos) for pos in range(lo, hi))
            if n < RHS:
                steps.append(("xch", n, lo, hi))
                begin = max(now, link_free.get("yp", 0.0))
                link_free["yp"] = begin + XCH_US * (hi - lo)
                arrive(link_free["yp"] + HOP_US, ("E", n, lo, hi))
            finish_ready()
        elif heap:
            now = max(now, heap[0][0])
        pump(now, LOOKAHEAD_US)
    assert not any(pools.values()) and len(finished) == RHS * XS
    return steps, now


def solution(mesh):
    depth_size = mesh.shape["depth"]
    mid = depth_size // 2
    steps, _ = plan(depth_size)

    def kernel(w_ref, x_ref, o_ref, a_all, x_all, acc, peer_acc, y_buf,
               a_ssem, a_rsem, x_ssem, x_rsem, d_ssem, d_rsem, t_ssem, t_rsem, e_ssem, e_rsem, y_ssem, y_rsem, l_sem):
        layer = lax.axis_index("depth")
        col = lax.axis_index("col")
        row = lax.axis_index("row")
        core = lax.rem(row, 2)
        xpos = row // 2
        rows, kcols = w_ref.shape
        unit = rows // 4
        hrows = rows // 2
        sub = x_ref.shape[2] // 4

        xh = xpos // 2
        yh = col // 2
        cross = lax.rem(xh + yh, 2)
        x_col = col + cross * (3 - 2 * col)

        def at(hops, y):
            return {"row": lax.rem(row + 2 * hops, 2 * XS), "col": y}

        sibling = {"row": row + 1 - 2 * core}
        links = {
            "x+": {"row": lax.rem(row + 2, 2 * XS)},
            "x-": {"row": lax.rem(row + 6, 2 * XS)},
            "ya": {"col": col + 1 - 2 * lax.rem(col, 2)},
            "yp": {"col": 3 - col},
            "z+": {"depth": lax.rem(layer + 1, depth_size)},
            "z-": {"depth": lax.rem(layer + depth_size - 1, depth_size)},
        }

        barrier = pltpu.get_barrier_semaphore()
        partners = [links["ya"], links["z+"], links["z-"], sibling]
        partners += [at(hops, col) for hops in range(1, XS)] + [at(hops, 3 - col) for hops in range(XS)]
        for partner in partners:
            pl.semaphore_signal(barrier, inc=1, device_id=partner, device_id_type=MESH)
        pl.semaphore_wait(barrier, len(partners))

        sent = []

        def a_index(name):
            return ((name[1] * 2 + name[2]) * 2 + name[3]) * 2 + name[4]

        def a_slot(name):
            _, dx, dp, half, piece = name
            return a_all.at[dp, pl.ds(POS[dx] * rows + half * hrows + piece * unit, unit), :]

        def x_index(name):
            return name[1] * (depth_size + 1) + (depth_size if name == ("XH", name[1], 1) else mid if name[0] == "XH" else name[2])

        def x_rows(core_idx, dz):
            start = (core_idx * depth_size + lax.rem(layer + depth_size - dz, depth_size)) * rows
            return pl.ds(pl.multiple_of(start, rows), rows)

        def x_slot(name):
            if name[0] == "XH":
                return x_all.at[name[1], name[2], x_rows(core, mid), :]
            return x_all.at[name[1], :, x_rows(core, name[2]), :]

        def x_out(src, there):
            if there[0] == "XH":
                return x_all.at[there[1], there[2], x_rows(core, src[2]), :]
            return x_slot(src)

        def remote(src, dst, ssem, rsem, device):
            copy = pltpu.make_async_remote_copy(src_ref=src, dst_ref=dst, send_sem=ssem, recv_sem=rsem, device_id=device, device_id_type=MESH)
            copy.start()
            sent.append(copy)

        def landed(slot, rsem):
            pltpu.make_async_remote_copy(src_ref=slot, dst_ref=slot, send_sem=l_sem.at[0], recv_sem=rsem, device_id=sibling, device_id_type=MESH).wait_recv()

        def columns(block):
            return pl.ds(pl.multiple_of(block * sub, sub), sub)

        own_a = pltpu.make_async_copy(w_ref, a_all.at[0, pl.ds(0, rows), :], l_sem.at[1])

        def exchange_x(r):
            s = lax.rem(xpos + x_col, 2)
            n = (1 - cross) * RHS + r
            for hops in (1, 3, 2, 0):
                src = x_ref.at[r, :, columns(lax.rem(xpos + hops, XS))]
                dst = x_all.at[n, s, x_rows(core, 0), :]
                ssem, rsem = t_ssem.at[r * XS + hops], t_rsem.at[n * 2 + s]
                if hops == 0:
                    pl.when(cross == 0)(lambda: pltpu.make_async_copy(src, dst, rsem).start())

                    @pl.when(cross == 1)
                    def _():
                        pltpu.make_async_remote_copy(src_ref=src, dst_ref=dst, send_sem=ssem, recv_sem=rsem, device_id=at(0, 3 - col), device_id_type=MESH).start()
                else:
                    remote(src, dst, ssem, rsem, at(hops, x_col))

        def matmul(n, lo, hi):
            kstep = min(2048, kcols)
            per = kcols // kstep

            def body(idx, carry):
                dp = idx // per
                k0 = pl.multiple_of(lax.rem(idx, per) * kstep, kstep)
                lhs = a_all[dp, pl.ds(lo * rows, (hi - lo) * rows), pl.ds(k0, kstep)]
                rhs = x_all[n, dp, pl.ds(k0, kstep), :]
                part = jnp.dot(lhs, rhs, preferred_element_type=jnp.float32)
                acc[n, pl.ds(lo, hi - lo)] += part.reshape(hi - lo, rows, sub)
                return carry

            lax.fori_loop(0, 2 * per, body, 0)

        def exchange_acc(n, lo, hi):
            span = pl.ds(lo, hi - lo)
            remote(acc.at[n, span], peer_acc.at[n, span], e_ssem.at[n * XS + lo], e_rsem.at[n * XS + lo], links["yp"])

        local = []

        def finish(r, pos):
            dx = next(d for d in POS if POS[d] == pos)
            y_buf[r, pos] = (acc[RHS + r, pos] + peer_acc[r, pos]).astype(y_buf.dtype)
            src, dst = y_buf.at[r, pos], o_ref.at[r, :, columns(xpos)]
            if dx == 0:
                copy = pltpu.make_async_copy(src, dst, y_ssem.at[r * XS])
                copy.start()
                local.append(copy)
            else:
                remote(src, dst, y_ssem.at[r * XS + dx], y_rsem.at[r * XS + dx], at(XS - dx, col))

        waited = set()
        for step in steps:
            if step[0] == "a2a":
                exchange_x(step[1])
                if step[1] == RHS - 1:
                    own_a.start()
                    acc[...] = jnp.zeros_like(acc)
            elif step[0] == "send":
                _, link, src, dst = step
                if dst[0] == "A":
                    if src[1:3] == (0, 0):
                        ref = w_ref.at[pl.ds(src[3] * hrows + src[4] * unit, unit), :]
                    else:
                        ref = a_slot(src)
                    idx = a_index(dst)
                    remote(ref, a_slot(dst), a_ssem.at[idx], a_rsem.at[idx], links[link])
                else:
                    idx = x_index(dst)
                    ref = x_out(src, dst)
                    remote(ref, ref, x_ssem.at[idx], x_rsem.at[idx], links[link])
            elif step[0] == "wait":
                name = step[1]
                if name[0] == "A":
                    landed(a_slot(name), a_rsem.at[a_index(name)])
                elif name[0] == "T":
                    for s in range(2):
                        landed(x_all.at[name[1], s, x_rows(core, 0), :], t_rsem.at[name[1] * 2 + s])
                else:
                    landed(x_slot(name), x_rsem.at[x_index(name)])
            elif step[0] == "share":
                _, n, dz = step
                slot = x_all.at[n, :, x_rows(core, dz), :]
                remote(slot, slot, d_ssem.at[n * depth_size + dz], d_rsem.at[n * depth_size + dz], sibling)
            elif step[0] == "mm":
                _, n, lo, hi = step
                if "a" not in waited:
                    waited.add("a")
                    own_a.wait()
                if n not in waited:
                    waited.add(n)
                    for dz in range(depth_size):
                        landed(x_all.at[n, :, x_rows(1 - core, dz), :], d_rsem.at[n * depth_size + dz])
                matmul(n, lo, hi)
            elif step[0] == "xch":
                exchange_acc(*step[1:])
            elif step[0] == "peer":
                _, n, lo, hi = step
                landed(peer_acc.at[n, pl.ds(lo, hi - lo)], e_rsem.at[n * XS + lo])
            else:
                finish(step[1], step[2])

        for r in range(RHS):
            for dx in range(1, XS):
                landed(o_ref.at[r, :, columns(lax.rem(xpos + dx, XS))], y_rsem.at[r * XS + dx])

            @pl.when(cross == 1)
            def _():
                src = x_ref.at[r, :, columns(xpos)]
                pltpu.make_async_remote_copy(src_ref=src, dst_ref=src, send_sem=t_ssem.at[r * XS], recv_sem=t_rsem.at[0], device_id=at(0, 3 - col), device_id_type=MESH).wait_send()
        for copy in local:
            copy.wait()
        for copy in sent:
            copy.wait_send()

    def local_product(w_local, x_local):
        rows, kcols = w_local.shape
        sub = x_local.shape[2] // 4
        dma = pltpu.SemaphoreType.DMA

        def sems(size):
            return [dma((size,)), dma((size,))]

        return pl.pallas_call(
            kernel,
            out_shape=jax.ShapeDtypeStruct(x_local.shape, jnp.bfloat16),
            in_specs=[pl.BlockSpec(memory_space=pl.ANY)] * 2,
            out_specs=pl.BlockSpec(memory_space=pl.ANY),
            scratch_shapes=[
                pltpu.VMEM((2, XS * rows, kcols), jnp.bfloat16),
                pltpu.VMEM((CHUNKS, 2, kcols, sub), jnp.bfloat16),
                pltpu.VMEM((CHUNKS, XS, rows, sub), jnp.float32),
                pltpu.VMEM((RHS, XS, rows, sub), jnp.float32),
                pltpu.VMEM((RHS, XS, rows, sub), jnp.bfloat16),
                *sems(32), *sems(CHUNKS * (depth_size + 1)), *sems(CHUNKS * depth_size),
                dma((RHS * XS,)), dma((CHUNKS * 2,)), *sems(RHS * XS), *sems(RHS * XS), dma((2,)),
            ],
            compiler_params=pltpu.CompilerParams(collective_id=0, has_side_effects=True, vmem_limit_bytes=67043328),
            cost_estimate=pl.CostEstimate(flops=2 * XS * rows * 2 * kcols * CHUNKS * sub, bytes_accessed=0, transcendentals=0),
            name="gather_matmul",
        )(w_local, x_local)

    return jax.shard_map(local_product, mesh=mesh, in_specs=(P(("row", "depth"), "col"), P(None, ("row", "depth"), "col")), out_specs=P(None, ("row", "depth"), "col"), check_vma=False)
```

```python
import heapq

import jax
import jax.numpy as jnp
from jax import lax
from jax.experimental import pallas as pl
from jax.experimental.pallas import tpu as pltpu
from jax.sharding import PartitionSpec as P

MESH = pl.DeviceIdType.MESH
XS = 4
YS = 4
RHS = 3
CHUNKS = 2 * RHS
ORDER = (0, 1, 2, 3, 4, 5)
POS = {0: 0, 1: 1, 3: 2, 2: 3}
READY = ((0,), (1,), (3,), (2,))

A_UNIT_US = 11.3
X_UNIT_US = 5.65
T_X_US = 5.65
T_Y_US = 11.3
HOLD_US = (0.0, 0.0, 0.0, 0.0, 30.0, 60.0)
A2A_AT_US = (0.0, 0.0, 0.0)
OUT_US = 2.8
D2D_US = 1.5
XCH_US = 5.65
HOP_US = 2.5
LOOKAHEAD_US = 2.0
BLOCK_US = 1.4
LATE_US = 0.0
LATE_E_US = 0.0


def a_sends(name):
    _, dx, dp, half, piece = name
    out = []

    def along_x():
        if dx == 0:
            out.append(("x+", ("A", 1, dp, half, piece)))
            out.append(("x-", ("A", 3, dp, half, piece)))
        elif dx == 1 and piece == 0:
            out.append(("x+", ("A", 2, dp, half, piece)))
        elif dx == 3 and piece == 1:
            out.append(("x-", ("A", 2, dp, half, piece)))

    if half == 0:
        if dp == 0:
            along_x()
            out.append(("ya", ("A", dx, 1, half, piece)))
    else:
        if dp == 0 and dx == 0:
            out.append(("ya", ("A", 0, 1, half, piece)))
        along_x()
    return out


def x_sends(name, depth_size):
    _, n, dz = name
    mid = depth_size // 2
    out = []
    if dz < mid:
        out.append(("z+", ("X", n, dz + 1) if dz + 1 < mid else ("XH", n, 0)))
    back = (depth_size - dz) % depth_size
    if back < mid:
        out.append(("z-", ("X", n, (dz - 1) % depth_size) if back + 1 < mid else ("XH", n, 1)))
    return out


def plan(depth_size):
    mid = depth_size // 2
    steps, heap, pools, link_free = [], [], {}, {}
    have = set()
    count = 0

    def arrive(when, name):
        nonlocal count
        if name[0] == "E":
            when += LATE_E_US
        elif name[0] == "P" or name[0] == "A" and not a_sends(name):
            when += LATE_US
        heapq.heappush(heap, (when, count, name))
        count += 1

    def cost(name):
        if name[0] == "A":
            return A_UNIT_US
        return X_UNIT_US if name[0] == "X" else X_UNIT_US / 2

    def priority(name):
        if name[0] == "A":
            return (next(i for i, g in enumerate(READY) if name[1] in g), name[4])
        return (ORDER.index(name[1]),)

    def pump(now, ahead):
        for link, pool in pools.items():
            while pool and link_free.get(link, 0.0) < now + ahead:
                pool.sort()
                _, _, src, dst = pool.pop(0)
                begin = max(now, link_free.get(link, 0.0))
                link_free[link] = begin + cost(dst)
                arrive(begin + cost(dst) + HOP_US, dst)
                steps.append(("send", link, src, dst))

    def offer(link, src, dst):
        nonlocal count
        pools.setdefault(link, []).append((priority(dst), count, src, dst))
        count += 1

    def got(name, now):
        have.add(name)
        if name[0] == "A":
            for link, there in a_sends(name):
                offer(link, name, there)
        elif name[0] in ("T", "X"):
            unit = ("X", name[1], 0) if name[0] == "T" else name
            for link, there in x_sends(unit, depth_size):
                offer(link, unit, there)
            share(name[1], unit[2], now)
        elif name[0] == "XH" and ("XH", name[1], 1 - name[2]) in have:
            share(name[1], mid, now)

    def share(n, dz, now):
        steps.append(("share", n, dz))
        arrive(now + D2D_US + HOP_US, ("P", n, dz))

    now = 0.0

    def take(link, when, spent):
        link_free[link] = max(when, link_free.get(link, 0.0)) + spent
        return link_free[link]

    def exchange(r):
        steps.append(("a2a", r))
        near = max(take("x+", now, T_X_US), take("x-", now, T_X_US)) + HOP_US
        arrive(max(near, HOLD_US[RHS + r]), ("T", RHS + r))
        arrive(max(take("yp", now, T_Y_US) + HOP_US + 1.0, near, HOLD_US[r]), ("T", r))

    exchange(0)
    for half, piece in ((0, 0), (1, 0), (0, 1), (1, 1)):
        got(("A", 0, 0, half, piece), now)
    pump(now, LOOKAHEAD_US)
    for r in range(1, RHS):
        arrive(A2A_AT_US[r], ("a2a", r))

    def a_need(pos):
        return set(("A", dx, dp, half, piece) for dx in POS if POS[dx] == pos for dp in range(2) for half in range(2) for piece in range(2))

    def x_need(n):
        out = set(("P", n, dz) for dz in range(depth_size))
        return out | set(("X", n, dz) for dz in range(1, depth_size) if dz != mid) | {("T", n), ("XH", n, 0), ("XH", n, 1)}

    left = [(n, pos) for n in ORDER for pos in range(XS)]
    made, arrived, finished = set(), set(), set()
    done = [0.0]

    def next_block():
        for n in ORDER:
            run = [pos for pos in range(XS) if (n, pos) in left and a_need(pos) <= have]
            if run and x_need(n) <= have:
                stop = run[0] + 1
                while stop in run:
                    stop += 1
                return n, run[0], stop
        return None

    def finish_ready():
        for r in range(RHS):
            for pos in range(XS):
                if (r, pos) in arrived and (RHS + r, pos) in made and (r, pos) not in finished:
                    finished.add((r, pos))
                    steps.append(("fin", r, pos))
                    for link in (("x-",), ("x+",), ("x+", "x-"))[pos - 1] if pos else ():
                        done[0] = max(done[0], take(link, now, OUT_US) + HOP_US)

    while heap or left:
        while heap and heap[0][0] <= now:
            _, _, name = heapq.heappop(heap)
            if name[0] == "a2a":
                exchange(name[1])
                continue
            if name[0] == "E":
                _, n, lo, hi = name
                steps.append(("peer", n, lo, hi))
                arrived |= set((n, pos) for pos in range(lo, hi))
                finish_ready()
                continue
            if name[0] != "P":
                steps.append(("wait", name))
            got(name, now)
            pump(now, LOOKAHEAD_US)
        block = next_block()
        if block is not None:
            n, lo, hi = block
            left = [b for b in left if b[0] != n or not lo <= b[1] < hi]
            spent = BLOCK_US * (hi - lo)
            pump(now, LOOKAHEAD_US + spent)
            steps.append(("mm", n, lo, hi))
            now += spent
            made |= set((n, pos) for pos in range(lo, hi))
            if n < RHS:
                steps.append(("xch", n, lo, hi))
                begin = max(now, link_free.get("yp", 0.0))
                link_free["yp"] = begin + XCH_US * (hi - lo)
                arrive(link_free["yp"] + HOP_US, ("E", n, lo, hi))
            finish_ready()
        elif heap:
            now = max(now, heap[0][0])
        pump(now, LOOKAHEAD_US)
    assert not any(pools.values()) and len(finished) == RHS * XS
    return steps, max(now, done[0])


def solution(mesh):
    depth_size = mesh.shape["depth"]
    mid = depth_size // 2
    steps, _ = plan(depth_size)

    def kernel(w_ref, x_ref, o_ref, a_all, x_all, acc, peer_acc, y_buf,
               a_ssem, a_rsem, x_ssem, x_rsem, d_ssem, d_rsem, t_ssem, t_rsem, e_ssem, e_rsem, y_ssem, y_rsem, l_sem):
        layer = lax.axis_index("depth")
        col = lax.axis_index("col")
        row = lax.axis_index("row")
        core = lax.rem(row, 2)
        xpos = row // 2
        rows, kcols = w_ref.shape
        unit = rows // 4
        hrows = rows // 2
        sub = x_ref.shape[2] // 4

        xh = xpos // 2
        yh = col // 2
        cross = lax.rem(xh + yh, 2)
        x_col = col + cross * (3 - 2 * col)

        def at(hops, y):
            return {"row": lax.rem(row + 2 * hops, 2 * XS), "col": y}

        sibling = {"row": row + 1 - 2 * core}
        links = {
            "x+": {"row": lax.rem(row + 2, 2 * XS)},
            "x-": {"row": lax.rem(row + 6, 2 * XS)},
            "ya": {"col": col + 1 - 2 * lax.rem(col, 2)},
            "yp": {"col": 3 - col},
            "z+": {"depth": lax.rem(layer + 1, depth_size)},
            "z-": {"depth": lax.rem(layer + depth_size - 1, depth_size)},
        }

        barrier = pltpu.get_barrier_semaphore()
        partners = [links["ya"], links["z+"], links["z-"], sibling]
        partners += [at(hops, col) for hops in range(1, XS)] + [at(hops, 3 - col) for hops in range(XS)]
        for partner in partners:
            pl.semaphore_signal(barrier, inc=1, device_id=partner, device_id_type=MESH)
        pl.semaphore_wait(barrier, len(partners))

        sent = []

        def a_index(name):
            return ((name[1] * 2 + name[2]) * 2 + name[3]) * 2 + name[4]

        def a_slot(name):
            _, dx, dp, half, piece = name
            return a_all.at[dp, pl.ds(POS[dx] * rows + half * hrows + piece * unit, unit), :]

        def x_index(name):
            return name[1] * (depth_size + 1) + (depth_size if name == ("XH", name[1], 1) else mid if name[0] == "XH" else name[2])

        def x_rows(core_idx, dz):
            start = (core_idx * depth_size + lax.rem(layer + depth_size - dz, depth_size)) * rows
            return pl.ds(pl.multiple_of(start, rows), rows)

        def x_slot(name):
            if name[0] == "XH":
                return x_all.at[name[1], name[2], x_rows(core, mid), :]
            return x_all.at[name[1], :, x_rows(core, name[2]), :]

        def x_out(src, there):
            if there[0] == "XH":
                return x_all.at[there[1], there[2], x_rows(core, src[2]), :]
            return x_slot(src)

        def remote(src, dst, ssem, rsem, device):
            copy = pltpu.make_async_remote_copy(src_ref=src, dst_ref=dst, send_sem=ssem, recv_sem=rsem, device_id=device, device_id_type=MESH)
            copy.start()
            sent.append(copy)

        def landed(slot, rsem):
            pltpu.make_async_remote_copy(src_ref=slot, dst_ref=slot, send_sem=l_sem.at[0], recv_sem=rsem, device_id=sibling, device_id_type=MESH).wait_recv()

        def columns(block):
            return pl.ds(pl.multiple_of(block * sub, sub), sub)

        own_a = pltpu.make_async_copy(w_ref, a_all.at[0, pl.ds(0, rows), :], l_sem.at[1])

        def exchange_x(r):
            s = lax.rem(xpos + x_col, 2)
            n = (1 - cross) * RHS + r
            for hops in (1, 3, 2, 0):
                src = x_ref.at[r, :, columns(lax.rem(xpos + hops, XS))]
                dst = x_all.at[n, s, x_rows(core, 0), :]
                ssem, rsem = t_ssem.at[r * XS + hops], t_rsem.at[n * 2 + s]
                if hops == 0:
                    pl.when(cross == 0)(lambda: pltpu.make_async_copy(src, dst, rsem).start())

                    @pl.when(cross == 1)
                    def _():
                        pltpu.make_async_remote_copy(src_ref=src, dst_ref=dst, send_sem=ssem, recv_sem=rsem, device_id=at(0, 3 - col), device_id_type=MESH).start()
                else:
                    remote(src, dst, ssem, rsem, at(hops, x_col))

        def matmul(n, lo, hi):
            kstep = min(2048, kcols)
            per = kcols // kstep

            def body(idx, carry):
                dp = idx // per
                k0 = pl.multiple_of(lax.rem(idx, per) * kstep, kstep)
                lhs = a_all[dp, pl.ds(lo * rows, (hi - lo) * rows), pl.ds(k0, kstep)]
                rhs = x_all[n, dp, pl.ds(k0, kstep), :]
                part = jnp.dot(lhs, rhs, preferred_element_type=jnp.float32)
                acc[n, pl.ds(lo, hi - lo)] += part.reshape(hi - lo, rows, sub)
                return carry

            lax.fori_loop(0, 2 * per, body, 0)

        def exchange_acc(n, lo, hi):
            span = pl.ds(lo, hi - lo)
            remote(acc.at[n, span], peer_acc.at[n, span], e_ssem.at[n * XS + lo], e_rsem.at[n * XS + lo], links["yp"])

        local = []

        def finish(r, pos):
            dx = next(d for d in POS if POS[d] == pos)
            y_buf[r, pos] = (acc[RHS + r, pos] + peer_acc[r, pos]).astype(y_buf.dtype)
            src, dst = y_buf.at[r, pos], o_ref.at[r, :, columns(xpos)]
            if dx == 0:
                copy = pltpu.make_async_copy(src, dst, y_ssem.at[r * XS])
                copy.start()
                local.append(copy)
            else:
                remote(src, dst, y_ssem.at[r * XS + dx], y_rsem.at[r * XS + dx], at(XS - dx, col))

        waited = set()
        for step in steps:
            if step[0] == "a2a":
                exchange_x(step[1])
                if step[1] == RHS - 1:
                    own_a.start()
                    acc[...] = jnp.zeros_like(acc)
            elif step[0] == "send":
                _, link, src, dst = step
                if dst[0] == "A":
                    if src[1:3] == (0, 0):
                        ref = w_ref.at[pl.ds(src[3] * hrows + src[4] * unit, unit), :]
                    else:
                        ref = a_slot(src)
                    idx = a_index(dst)
                    remote(ref, a_slot(dst), a_ssem.at[idx], a_rsem.at[idx], links[link])
                else:
                    idx = x_index(dst)
                    ref = x_out(src, dst)
                    remote(ref, ref, x_ssem.at[idx], x_rsem.at[idx], links[link])
            elif step[0] == "wait":
                name = step[1]
                if name[0] == "A":
                    landed(a_slot(name), a_rsem.at[a_index(name)])
                elif name[0] == "T":
                    for s in range(2):
                        landed(x_all.at[name[1], s, x_rows(core, 0), :], t_rsem.at[name[1] * 2 + s])
                else:
                    landed(x_slot(name), x_rsem.at[x_index(name)])
            elif step[0] == "share":
                _, n, dz = step
                slot = x_all.at[n, :, x_rows(core, dz), :]
                remote(slot, slot, d_ssem.at[n * depth_size + dz], d_rsem.at[n * depth_size + dz], sibling)
            elif step[0] == "mm":
                _, n, lo, hi = step
                if "a" not in waited:
                    waited.add("a")
                    own_a.wait()
                if n not in waited:
                    waited.add(n)
                    for dz in range(depth_size):
                        landed(x_all.at[n, :, x_rows(1 - core, dz), :], d_rsem.at[n * depth_size + dz])
                matmul(n, lo, hi)
            elif step[0] == "xch":
                exchange_acc(*step[1:])
            elif step[0] == "peer":
                _, n, lo, hi = step
                landed(peer_acc.at[n, pl.ds(lo, hi - lo)], e_rsem.at[n * XS + lo])
            else:
                finish(step[1], step[2])

        for r in range(RHS):
            for dx in range(1, XS):
                landed(o_ref.at[r, :, columns(lax.rem(xpos + dx, XS))], y_rsem.at[r * XS + dx])

            @pl.when(cross == 1)
            def _():
                src = x_ref.at[r, :, columns(xpos)]
                pltpu.make_async_remote_copy(src_ref=src, dst_ref=src, send_sem=t_ssem.at[r * XS], recv_sem=t_rsem.at[0], device_id=at(0, 3 - col), device_id_type=MESH).wait_send()
        for copy in local:
            copy.wait()
        for copy in sent:
            copy.wait_send()

    def local_product(w_local, x_local):
        rows, kcols = w_local.shape
        sub = x_local.shape[2] // 4
        dma = pltpu.SemaphoreType.DMA

        def sems(size):
            return [dma((size,)), dma((size,))]

        return pl.pallas_call(
            kernel,
            out_shape=jax.ShapeDtypeStruct(x_local.shape, jnp.bfloat16),
            in_specs=[pl.BlockSpec(memory_space=pl.ANY)] * 2,
            out_specs=pl.BlockSpec(memory_space=pl.ANY),
            scratch_shapes=[
                pltpu.VMEM((2, XS * rows, kcols), jnp.bfloat16),
                pltpu.VMEM((CHUNKS, 2, kcols, sub), jnp.bfloat16),
                pltpu.VMEM((CHUNKS, XS, rows, sub), jnp.float32),
                pltpu.VMEM((RHS, XS, rows, sub), jnp.float32),
                pltpu.VMEM((RHS, XS, rows, sub), jnp.bfloat16),
                *sems(32), *sems(CHUNKS * (depth_size + 1)), *sems(CHUNKS * depth_size),
                dma((RHS * XS,)), dma((CHUNKS * 2,)), *sems(RHS * XS), *sems(RHS * XS), dma((2,)),
            ],
            compiler_params=pltpu.CompilerParams(collective_id=0, has_side_effects=True, vmem_limit_bytes=67043328),
            cost_estimate=pl.CostEstimate(flops=2 * XS * rows * 2 * kcols * CHUNKS * sub, bytes_accessed=0, transcendentals=0),
            name="gather_matmul",
        )(w_local, x_local)

    return jax.shard_map(local_product, mesh=mesh, in_specs=(P(("row", "depth"), "col"), P(None, ("row", "depth"), "col")), out_specs=P(None, ("row", "depth"), "col"), check_vma=False)
```

```python
import heapq

import jax
import jax.numpy as jnp
from jax import lax
from jax.experimental import pallas as pl
from jax.experimental.pallas import tpu as pltpu
from jax.sharding import PartitionSpec as P

MESH = pl.DeviceIdType.MESH
XS = 4
YS = 4
RHS = 3
CHUNKS = 2 * RHS
ORDER = (0, 1, 2, 3, 4, 5)
BLOCKS = 2 * XS
FINE = 8
POS = {0: 0, 1: 1, 3: 2, 2: 3}
READY = ((0,), (1,), (2,), (3,))

A_UNIT_US = 11.3
X_UNIT_US = 5.65
T_X_US = 5.65
T_Y_US = 11.3
HOLD_US = (0.0, 0.0, 0.0, 9, 55, 66)
A2A_AT_US = (0.0, 0.0, 24.4)
OUT_US = 1.41
D2D_US = 1.5
XCH_US = 2.83
HOP_US = 2.5
AHEAD_A_US = 2.4
AHEAD_X_US = 2.5
A_WEIGHTS = (1.3, 0.06, 0.78, -0.71)
X_WEIGHTS = (0.4, 0.33)
BLOCK_US = 0.55
BLOCK0_US = 0.4
LATE_US = 0.0
LATE_E_US = 0.0


def a_sends(name):
    _, dx, dp, half, piece = name
    out = []

    def along_x():
        if dx == 0:
            out.append(("x+", ("A", 1, dp, half, piece)))
            out.append(("x-", ("A", 3, dp, half, piece)))
        elif dx == 1 and piece == 0:
            out.append(("x+", ("A", 2, dp, half, piece)))
        elif dx == 3 and piece == 1:
            out.append(("x-", ("A", 2, dp, half, piece)))

    if half == 0:
        if dp == 0:
            along_x()
            out.append(("ya", ("A", dx, 1, half, piece)))
    else:
        if dp == 0 and dx == 0:
            out.append(("ya", ("A", 0, 1, half, piece)))
        along_x()
    return out


def x_sends(name, depth_size):
    _, n, dz = name
    mid = depth_size // 2
    out = []
    if dz < mid:
        out.append(("z+", ("X", n, dz + 1) if dz + 1 < mid else ("XH", n, 0)))
    back = (depth_size - dz) % depth_size
    if back < mid:
        out.append(("z-", ("X", n, (dz - 1) % depth_size) if back + 1 < mid else ("XH", n, 1)))
    return out


def plan(depth_size):
    mid = depth_size // 2
    steps, heap, pools, link_free = [], [], {}, {}
    have = set()
    count = 0

    def arrive(when, name):
        nonlocal count
        if name[0] == "E":
            when += LATE_E_US
        elif name[0] == "P" or name[0] == "A" and not a_sends(name):
            when += LATE_US
        heapq.heappush(heap, (when, count, name))
        count += 1

    def cost(name):
        if name[0] == "A":
            return A_UNIT_US
        return X_UNIT_US if name[0] == "X" else X_UNIT_US / 2

    def priority(name):
        if name[0] == "A":
            parts = (next(i for i, g in enumerate(READY) if name[1] in g), name[3], name[2], name[4])
            return sum(w * p for w, p in zip(A_WEIGHTS, parts))
        away = mid if name[0] == "XH" else min(name[2], depth_size - name[2])
        return X_WEIGHTS[0] * ORDER.index(name[1]) + X_WEIGHTS[1] * away

    def pump(now, spent):
        for link, pool in pools.items():
            ahead = spent + (AHEAD_X_US if link[0] == "z" else AHEAD_A_US)
            while pool and link_free.get(link, 0.0) < now + ahead:
                pool.sort()
                _, _, src, dst = pool.pop(0)
                begin = max(now, link_free.get(link, 0.0))
                link_free[link] = begin + cost(dst)
                arrive(begin + cost(dst) + HOP_US, dst)
                steps.append(("send", link, src, dst))

    def offer(link, src, dst):
        nonlocal count
        pools.setdefault(link, []).append((priority(dst), count, src, dst))
        count += 1

    def got(name, now):
        have.add(name)
        if name[0] == "A":
            for link, there in a_sends(name):
                offer(link, name, there)
        elif name[0] in ("T", "X"):
            unit = ("X", name[1], 0) if name[0] == "T" else name
            for link, there in x_sends(unit, depth_size):
                offer(link, unit, there)
            share(name[1], unit[2], now)
        elif name[0] == "XH" and ("XH", name[1], 1 - name[2]) in have:
            share(name[1], mid, now)

    def share(n, dz, now):
        steps.append(("share", n, dz))
        arrive(now + D2D_US + HOP_US, ("P", n, dz))

    now = 0.0

    def take(link, when, spent):
        link_free[link] = max(when, link_free.get(link, 0.0)) + spent
        return link_free[link]

    def exchange(r):
        steps.append(("a2a", r))
        near = max(take("x+", now, T_X_US), take("x-", now, T_X_US)) + HOP_US
        arrive(max(near, HOLD_US[RHS + r]), ("T", RHS + r))
        arrive(max(take("yp", now, T_Y_US) + HOP_US + 1.0, near, HOLD_US[r]), ("T", r))

    exchange(0)
    for half, piece in ((0, 0), (1, 0), (0, 1), (1, 1)):
        got(("A", 0, 0, half, piece), now)
    pump(now, 0.0)
    for r in range(1, RHS):
        arrive(A2A_AT_US[r], ("a2a", r))

    def a_need(pos):
        return set(("A", dx, dp, pos % 2, piece) for dx in POS if POS[dx] == pos // 2 for dp in range(2) for piece in range(2))

    def x_need(n):
        out = set(("P", n, dz) for dz in range(depth_size))
        return out | set(("X", n, dz) for dz in range(1, depth_size) if dz != mid) | {("T", n), ("XH", n, 0), ("XH", n, 1)}

    left = [(n, pos) for n in ORDER for pos in range(BLOCKS)]
    made, arrived, finished = set(), set(), set()
    done = [0.0]

    def next_block():
        for n in ORDER:
            run = [pos for pos in range(BLOCKS) if (n, pos) in left and a_need(pos) <= have]
            if not run or not x_need(n) <= have:
                continue
            stop = run[0] + 1
            while stop in run:
                stop += 1
            if run[0] < FINE and (run[0] % 2 or stop - run[0] < 2):
                continue
            if stop % 2 and stop <= FINE:
                stop -= 1
            return n, run[0], stop
        return None

    def finish_ready():
        for r in range(RHS):
            for pos in range(BLOCKS):
                if (r, pos) in arrived and (RHS + r, pos) in made and (r, pos) not in finished:
                    finished.add((r, pos))
                    steps.append(("fin", r, pos))
                    for link in (("x-",), ("x+",), ("x+", "x-"))[pos // 2 - 1] if pos > 1 else ():
                        done[0] = max(done[0], take(link, now, OUT_US) + HOP_US)

    while heap or left:
        while heap and heap[0][0] <= now:
            _, _, name = heapq.heappop(heap)
            if name[0] == "a2a":
                exchange(name[1])
                continue
            if name[0] == "E":
                _, n, lo, hi = name
                steps.append(("peer", n, lo, hi))
                arrived |= set((n, pos) for pos in range(lo, hi))
                finish_ready()
                continue
            if name[0] != "P":
                steps.append(("wait", name))
            got(name, now)
            pump(now, 0.0)
        block = next_block()
        if block is not None:
            n, lo, hi = block
            left = [b for b in left if b[0] != n or not lo <= b[1] < hi]
            spent = BLOCK_US * (hi - lo) + BLOCK0_US
            pump(now, spent)
            steps.append(("mm", n, lo, hi))
            now += spent
            made |= set((n, pos) for pos in range(lo, hi))
            if n < RHS:
                steps.append(("xch", n, lo, hi))
                begin = max(now, link_free.get("yp", 0.0))
                link_free["yp"] = begin + XCH_US * (hi - lo)
                arrive(link_free["yp"] + HOP_US, ("E", n, lo, hi))
            finish_ready()
        elif heap:
            now = max(now, heap[0][0])
        pump(now, 0.0)
    assert not any(pools.values()) and len(finished) == RHS * BLOCKS
    return steps, max(now, done[0])


def solution(mesh):
    depth_size = mesh.shape["depth"]
    mid = depth_size // 2
    steps, _ = plan(depth_size)

    def kernel(w_ref, x_ref, o_ref, a_all, x_all, acc, peer_acc, y_buf,
               a_ssem, a_rsem, x_ssem, x_rsem, d_ssem, d_rsem, t_ssem, t_rsem, e_ssem, e_rsem, y_ssem, y_rsem, l_sem):
        layer = lax.axis_index("depth")
        col = lax.axis_index("col")
        row = lax.axis_index("row")
        core = lax.rem(row, 2)
        xpos = row // 2
        rows, kcols = w_ref.shape
        unit = rows // 4
        hrows = rows // 2
        sub = x_ref.shape[2] // 4

        xh = xpos // 2
        yh = col // 2
        cross = lax.rem(xh + yh, 2)
        x_col = col + cross * (3 - 2 * col)

        def at(hops, y):
            return {"row": lax.rem(row + 2 * hops, 2 * XS), "col": y}

        sibling = {"row": row + 1 - 2 * core}
        links = {
            "x+": {"row": lax.rem(row + 2, 2 * XS)},
            "x-": {"row": lax.rem(row + 6, 2 * XS)},
            "ya": {"col": col + 1 - 2 * lax.rem(col, 2)},
            "yp": {"col": 3 - col},
            "z+": {"depth": lax.rem(layer + 1, depth_size)},
            "z-": {"depth": lax.rem(layer + depth_size - 1, depth_size)},
        }

        barrier = pltpu.get_barrier_semaphore()
        partners = [links["ya"], links["z+"], links["z-"], sibling]
        partners += [at(hops, col) for hops in range(1, XS)] + [at(hops, 3 - col) for hops in range(XS)]
        for partner in partners:
            pl.semaphore_signal(barrier, inc=1, device_id=partner, device_id_type=MESH)
        pl.semaphore_wait(barrier, len(partners))

        sent = []

        def a_index(name):
            return ((name[1] * 2 + name[2]) * 2 + name[3]) * 2 + name[4]

        def a_slot(name):
            _, dx, dp, half, piece = name
            return a_all.at[pl.ds(POS[dx] * rows + half * hrows + piece * unit, unit), pl.ds(dp * kcols, kcols)]

        def x_index(name):
            return name[1] * (depth_size + 1) + (depth_size if name == ("XH", name[1], 1) else mid if name[0] == "XH" else name[2])

        def x_rows(core_idx, dz):
            start = (core_idx * depth_size + lax.rem(layer + depth_size - dz, depth_size)) * rows
            return pl.ds(pl.multiple_of(start, rows), rows)

        def x_slot(name):
            if name[0] == "XH":
                return x_all.at[name[1], name[2], x_rows(core, mid), :]
            return x_all.at[name[1], :, x_rows(core, name[2]), :]

        def x_out(src, there):
            if there[0] == "XH":
                return x_all.at[there[1], there[2], x_rows(core, src[2]), :]
            return x_slot(src)

        def remote(src, dst, ssem, rsem, device):
            copy = pltpu.make_async_remote_copy(src_ref=src, dst_ref=dst, send_sem=ssem, recv_sem=rsem, device_id=device, device_id_type=MESH)
            copy.start()
            sent.append(copy)

        def landed(slot, rsem):
            pltpu.make_async_remote_copy(src_ref=slot, dst_ref=slot, send_sem=l_sem.at[0], recv_sem=rsem, device_id=sibling, device_id_type=MESH).wait_recv()

        def columns(block):
            return pl.ds(pl.multiple_of(block * sub, sub), sub)

        own_a = pltpu.make_async_copy(w_ref, a_all.at[pl.ds(0, rows), pl.ds(0, kcols)], l_sem.at[1])

        def exchange_x(r):
            s = lax.rem(xpos + x_col, 2)
            n = (1 - cross) * RHS + r
            for hops in (1, 3, 2, 0):
                src = x_ref.at[r, :, columns(lax.rem(xpos + hops, XS))]
                dst = x_all.at[n, s, x_rows(core, 0), :]
                ssem, rsem = t_ssem.at[r * XS + hops], t_rsem.at[n * 2 + s]
                if hops == 0:
                    pl.when(cross == 0)(lambda: pltpu.make_async_copy(src, dst, rsem).start())

                    @pl.when(cross == 1)
                    def _():
                        pltpu.make_async_remote_copy(src_ref=src, dst_ref=dst, send_sem=ssem, recv_sem=rsem, device_id=at(0, 3 - col), device_id_type=MESH).start()
                else:
                    remote(src, dst, ssem, rsem, at(hops, x_col))

        def matmul(n, lo, hi):
            kstep = kcols if hi - lo <= 4 else kcols // 2

            def body(idx, carry):
                k0 = pl.multiple_of(idx * kstep, kstep)
                lhs = a_all[pl.ds(lo * hrows, (hi - lo) * hrows), pl.ds(k0, kstep)]
                rhs = x_all[n, idx // (kcols // kstep), pl.ds(pl.multiple_of(lax.rem(k0, kcols), kstep), kstep), :]
                prod = jnp.dot(lhs, rhs, preferred_element_type=jnp.float32)
                acc[n, pl.ds(lo, hi - lo)] += prod.reshape(hi - lo, hrows, sub)
                return carry

            lax.fori_loop(0, 2 * kcols // kstep, body, 0)

        def exchange_acc(n, lo, hi):
            span = pl.ds(lo, hi - lo)
            remote(acc.at[n, span], peer_acc.at[n, span], e_ssem.at[n * BLOCKS + lo], e_rsem.at[n * BLOCKS + lo], links["yp"])

        local = []

        def finish(r, pos):
            dx = next(d for d in POS if POS[d] == pos // 2)
            half = pos % 2
            y_buf[r, pos] = (acc[RHS + r, pos] + peer_acc[r, pos]).astype(y_buf.dtype)
            src, dst = y_buf.at[r, pos], o_ref.at[r, pl.ds(half * hrows, hrows), columns(xpos)]
            sem = (r * XS + dx) * 2 + half
            if dx == 0:
                copy = pltpu.make_async_copy(src, dst, y_ssem.at[sem])
                copy.start()
                local.append(copy)
            else:
                remote(src, dst, y_ssem.at[sem], y_rsem.at[sem], at(XS - dx, col))

        waited = set()
        for step in steps:
            if step[0] == "a2a":
                exchange_x(step[1])
                if step[1] == RHS - 1:
                    own_a.start()
                    acc[...] = jnp.zeros_like(acc)
            elif step[0] == "send":
                _, link, src, dst = step
                if dst[0] == "A":
                    if src[1:3] == (0, 0):
                        ref = w_ref.at[pl.ds(src[3] * hrows + src[4] * unit, unit), :]
                    else:
                        ref = a_slot(src)
                    idx = a_index(dst)
                    remote(ref, a_slot(dst), a_ssem.at[idx], a_rsem.at[idx], links[link])
                else:
                    idx = x_index(dst)
                    ref = x_out(src, dst)
                    remote(ref, ref, x_ssem.at[idx], x_rsem.at[idx], links[link])
            elif step[0] == "wait":
                name = step[1]
                if name[0] == "A":
                    landed(a_slot(name), a_rsem.at[a_index(name)])
                elif name[0] == "T":
                    for s in range(2):
                        landed(x_all.at[name[1], s, x_rows(core, 0), :], t_rsem.at[name[1] * 2 + s])
                else:
                    landed(x_slot(name), x_rsem.at[x_index(name)])
            elif step[0] == "share":
                _, n, dz = step
                slot = x_all.at[n, :, x_rows(core, dz), :]
                remote(slot, slot, d_ssem.at[n * depth_size + dz], d_rsem.at[n * depth_size + dz], sibling)
            elif step[0] == "mm":
                _, n, lo, hi = step
                if "a" not in waited:
                    waited.add("a")
                    own_a.wait()
                if n not in waited:
                    waited.add(n)
                    for dz in range(depth_size):
                        landed(x_all.at[n, :, x_rows(1 - core, dz), :], d_rsem.at[n * depth_size + dz])
                matmul(n, lo, hi)
            elif step[0] == "xch":
                exchange_acc(*step[1:])
            elif step[0] == "peer":
                _, n, lo, hi = step
                landed(peer_acc.at[n, pl.ds(lo, hi - lo)], e_rsem.at[n * BLOCKS + lo])
            else:
                finish(step[1], step[2])

        for r in range(RHS):
            for dx in range(1, XS):
                for half in range(2):
                    slot = o_ref.at[r, pl.ds(half * hrows, hrows), columns(lax.rem(xpos + dx, XS))]
                    landed(slot, y_rsem.at[(r * XS + dx) * 2 + half])

            @pl.when(cross == 1)
            def _():
                src = x_ref.at[r, :, columns(xpos)]
                pltpu.make_async_remote_copy(src_ref=src, dst_ref=src, send_sem=t_ssem.at[r * XS], recv_sem=t_rsem.at[0], device_id=at(0, 3 - col), device_id_type=MESH).wait_send()
        for copy in local:
            copy.wait()
        for copy in sent:
            copy.wait_send()

    def local_product(w_local, x_local):
        rows, kcols = w_local.shape
        sub = x_local.shape[2] // 4
        dma = pltpu.SemaphoreType.DMA

        def sems(size):
            return [dma((size,)), dma((size,))]

        return pl.pallas_call(
            kernel,
            out_shape=jax.ShapeDtypeStruct(x_local.shape, jnp.bfloat16),
            in_specs=[pl.BlockSpec(memory_space=pl.ANY)] * 2,
            out_specs=pl.BlockSpec(memory_space=pl.ANY),
            scratch_shapes=[
                pltpu.VMEM((XS * rows, 2 * kcols), jnp.bfloat16),
                pltpu.VMEM((CHUNKS, 2, kcols, sub), jnp.bfloat16),
                pltpu.VMEM((CHUNKS, BLOCKS, rows // 2, sub), jnp.float32),
                pltpu.VMEM((RHS, BLOCKS, rows // 2, sub), jnp.float32),
                pltpu.VMEM((RHS, BLOCKS, rows // 2, sub), jnp.bfloat16),
                *sems(32), *sems(CHUNKS * (depth_size + 1)), *sems(CHUNKS * depth_size),
                dma((RHS * XS,)), dma((CHUNKS * 2,)), *sems(RHS * BLOCKS), *sems(RHS * BLOCKS), dma((2,)),
            ],
            compiler_params=pltpu.CompilerParams(collective_id=0, has_side_effects=True, vmem_limit_bytes=67043328),
            cost_estimate=pl.CostEstimate(flops=2 * XS * rows * 2 * kcols * CHUNKS * sub, bytes_accessed=0, transcendentals=0),
            name="gather_matmul",
        )(w_local, x_local)

    return jax.shard_map(local_product, mesh=mesh, in_specs=(P(("row", "depth"), "col"), P(None, ("row", "depth"), "col")), out_specs=P(None, ("row", "depth"), "col"), check_vma=False)
```

```python
import heapq

import jax
import jax.numpy as jnp
from jax import lax
from jax.experimental import pallas as pl
from jax.experimental.pallas import tpu as pltpu
from jax.sharding import PartitionSpec as P

MESH = pl.DeviceIdType.MESH
XS = 4
YS = 4
RHS = 3
CHUNKS = 2 * RHS
ORDER = (0, 1, 2, 3, 4, 5)
BLOCKS = 2 * XS
FINE = 6
POS = {0: 0, 1: 1, 3: 2, 2: 3}
READY = ((0,), (1, 3), (2,))

A_UNIT_US = 11.3
X_UNIT_US = 5.65
T_X_US = 5.65
T_Y_US = 11.3
HOLD_US = (0.0, 0.0, 0.0, 0.0, 37, 98)
A2A_AT_US = (0.0, 4.6, 5.2)
OUT_US = 1.41
D2D_US = 1.5
XCH_US = 2.83
HOP_US = 2.8
AHEAD_A_US = 1.1
AHEAD_X_US = 2.7
A_WEIGHTS = (0.96, 0.31, 0.16, -0.76)
X_WEIGHTS = (0.57, 0.04)
BLOCK_US = 0.55
BLOCK0_US = 0.4
LATE_US = 0.0
LATE_E_US = 0.0


def a_sends(name):
    _, dx, dp, half, piece = name
    out = []

    def along_x():
        if dx == 0:
            out.append(("x+", ("A", 1, dp, half, piece)))
            out.append(("x-", ("A", 3, dp, half, piece)))
        elif dx == 1 and piece == 0:
            out.append(("x+", ("A", 2, dp, half, piece)))
        elif dx == 3 and piece == 1:
            out.append(("x-", ("A", 2, dp, half, piece)))

    if half == 0:
        if dp == 0:
            along_x()
            out.append(("ya", ("A", dx, 1, half, piece)))
    else:
        if dp == 0 and dx == 0:
            out.append(("ya", ("A", 0, 1, half, piece)))
        along_x()
    return out


def x_sends(name, depth_size):
    _, n, dz = name
    mid = depth_size // 2
    out = []
    if dz < mid:
        out.append(("z+", ("X", n, dz + 1) if dz + 1 < mid else ("XH", n, 0)))
    back = (depth_size - dz) % depth_size
    if back < mid:
        out.append(("z-", ("X", n, (dz - 1) % depth_size) if back + 1 < mid else ("XH", n, 1)))
    return out


def plan(depth_size):
    mid = depth_size // 2
    steps, heap, pools, link_free = [], [], {}, {}
    have = set()
    count = 0

    def arrive(when, name):
        nonlocal count
        if name[0] == "E":
            when += LATE_E_US
        elif name[0] == "P" or name[0] == "A" and not a_sends(name):
            when += LATE_US
        heapq.heappush(heap, (when, count, name))
        count += 1

    def cost(name):
        if name[0] == "A":
            return A_UNIT_US
        return X_UNIT_US if name[0] == "X" else X_UNIT_US / 2

    def priority(name):
        if name[0] == "A":
            parts = (next(i for i, g in enumerate(READY) if name[1] in g), name[3], name[2], name[4])
            return sum(w * p for w, p in zip(A_WEIGHTS, parts))
        away = mid if name[0] == "XH" else min(name[2], depth_size - name[2])
        return X_WEIGHTS[0] * ORDER.index(name[1]) + X_WEIGHTS[1] * away

    def pump(now, spent):
        for link, pool in pools.items():
            ahead = spent + (AHEAD_X_US if link[0] == "z" else AHEAD_A_US)
            while pool and link_free.get(link, 0.0) < now + ahead:
                pool.sort()
                _, _, src, dst = pool.pop(0)
                begin = max(now, link_free.get(link, 0.0))
                link_free[link] = begin + cost(dst)
                arrive(begin + cost(dst) + HOP_US, dst)
                steps.append(("send", link, src, dst))

    def offer(link, src, dst):
        nonlocal count
        pools.setdefault(link, []).append((priority(dst), count, src, dst))
        count += 1

    def got(name, now):
        have.add(name)
        if name[0] == "A":
            for link, there in a_sends(name):
                offer(link, name, there)
        elif name[0] in ("T", "X"):
            unit = ("X", name[1], 0) if name[0] == "T" else name
            for link, there in x_sends(unit, depth_size):
                offer(link, unit, there)
            share(name[1], unit[2], now)
        elif name[0] == "XH" and ("XH", name[1], 1 - name[2]) in have:
            share(name[1], mid, now)

    def share(n, dz, now):
        steps.append(("share", n, dz))
        arrive(now + D2D_US + HOP_US, ("P", n, dz))

    now = 0.0

    def take(link, when, spent):
        link_free[link] = max(when, link_free.get(link, 0.0)) + spent
        return link_free[link]

    def exchange(r):
        steps.append(("a2a", r))
        near = max(take("x+", now, T_X_US), take("x-", now, T_X_US)) + HOP_US
        arrive(max(near, HOLD_US[RHS + r]), ("T", RHS + r))
        arrive(max(take("yp", now, T_Y_US) + HOP_US + 1.0, near, HOLD_US[r]), ("T", r))

    exchange(0)
    for half, piece in ((0, 0), (1, 0), (0, 1), (1, 1)):
        got(("A", 0, 0, half, piece), now)
    pump(now, 0.0)
    for r in range(1, RHS):
        arrive(A2A_AT_US[r], ("a2a", r))

    def a_need(pos):
        return set(("A", dx, dp, pos % 2, piece) for dx in POS if POS[dx] == pos // 2 for dp in range(2) for piece in range(2))

    def x_need(n):
        out = set(("P", n, dz) for dz in range(depth_size))
        return out | set(("X", n, dz) for dz in range(1, depth_size) if dz != mid) | {("T", n), ("XH", n, 0), ("XH", n, 1)}

    left = [(n, pos) for n in ORDER for pos in range(BLOCKS)]
    made, arrived, finished = set(), set(), set()
    done = [0.0]

    def next_block():
        for n in ORDER:
            run = [pos for pos in range(BLOCKS) if (n, pos) in left and a_need(pos) <= have]
            if not run or not x_need(n) <= have:
                continue
            stop = run[0] + 1
            while stop in run:
                stop += 1
            if run[0] < FINE and (run[0] % 2 or stop - run[0] < 2):
                continue
            if stop % 2 and stop <= FINE:
                stop -= 1
            return n, run[0], stop
        return None

    def finish_ready():
        for r in range(RHS):
            for pos in range(BLOCKS):
                if (r, pos) in arrived and (RHS + r, pos) in made and (r, pos) not in finished:
                    finished.add((r, pos))
                    steps.append(("fin", r, pos))
                    for link in (("x-",), ("x+",), ("x+", "x-"))[pos // 2 - 1] if pos > 1 else ():
                        done[0] = max(done[0], take(link, now, OUT_US) + HOP_US)

    while heap or left:
        while heap and heap[0][0] <= now:
            _, _, name = heapq.heappop(heap)
            if name[0] == "a2a":
                exchange(name[1])
                continue
            if name[0] == "E":
                _, n, lo, hi = name
                steps.append(("peer", n, lo, hi))
                arrived |= set((n, pos) for pos in range(lo, hi))
                finish_ready()
                continue
            if name[0] != "P":
                steps.append(("wait", name))
            got(name, now)
            pump(now, 0.0)
        block = next_block()
        if block is not None:
            n, lo, hi = block
            left = [b for b in left if b[0] != n or not lo <= b[1] < hi]
            spent = BLOCK_US * (hi - lo) + BLOCK0_US
            pump(now, spent)
            steps.append(("mm", n, lo, hi))
            now += spent
            made |= set((n, pos) for pos in range(lo, hi))
            if n < RHS:
                steps.append(("xch", n, lo, hi))
                begin = max(now, link_free.get("yp", 0.0))
                link_free["yp"] = begin + XCH_US * (hi - lo)
                arrive(link_free["yp"] + HOP_US, ("E", n, lo, hi))
            finish_ready()
        elif heap:
            now = max(now, heap[0][0])
        pump(now, 0.0)
    assert not any(pools.values()) and len(finished) == RHS * BLOCKS
    return steps, max(now, done[0])


def solution(mesh):
    depth_size = mesh.shape["depth"]
    mid = depth_size // 2
    steps, _ = plan(depth_size)

    def kernel(w_ref, x_ref, o_ref, a_all, x_all, acc, peer_acc, y_buf,
               a_ssem, a_rsem, x_ssem, x_rsem, d_ssem, d_rsem, t_ssem, t_rsem, e_ssem, e_rsem, y_ssem, y_rsem, l_sem):
        layer = lax.axis_index("depth")
        col = lax.axis_index("col")
        row = lax.axis_index("row")
        core = lax.rem(row, 2)
        xpos = row // 2
        rows, kcols = w_ref.shape
        unit = rows // 4
        hrows = rows // 2
        sub = x_ref.shape[2] // 4

        xh = xpos // 2
        yh = col // 2
        cross = lax.rem(xh + yh, 2)
        x_col = col + cross * (3 - 2 * col)

        def at(hops, y):
            return {"row": lax.rem(row + 2 * hops, 2 * XS), "col": y}

        sibling = {"row": row + 1 - 2 * core}
        links = {
            "x+": {"row": lax.rem(row + 2, 2 * XS)},
            "x-": {"row": lax.rem(row + 6, 2 * XS)},
            "ya": {"col": col + 1 - 2 * lax.rem(col, 2)},
            "yp": {"col": 3 - col},
            "z+": {"depth": lax.rem(layer + 1, depth_size)},
            "z-": {"depth": lax.rem(layer + depth_size - 1, depth_size)},
        }

        barrier = pltpu.get_barrier_semaphore()
        partners = [links["ya"], links["z+"], links["z-"], sibling]
        partners += [at(hops, col) for hops in range(1, XS)] + [at(hops, 3 - col) for hops in range(XS)]
        for partner in partners:
            pl.semaphore_signal(barrier, inc=1, device_id=partner, device_id_type=MESH)
        pl.semaphore_wait(barrier, len(partners))

        sent = []

        def a_index(name):
            return ((name[1] * 2 + name[2]) * 2 + name[3]) * 2 + name[4]

        def a_slot(name):
            _, dx, dp, half, piece = name
            return a_all.at[pl.ds(POS[dx] * rows + half * hrows + piece * unit, unit), pl.ds(dp * kcols, kcols)]

        def x_index(name):
            return name[1] * (depth_size + 1) + (depth_size if name == ("XH", name[1], 1) else mid if name[0] == "XH" else name[2])

        def x_rows(core_idx, dz):
            start = (core_idx * depth_size + lax.rem(layer + depth_size - dz, depth_size)) * rows
            return pl.ds(pl.multiple_of(start, rows), rows)

        def x_slot(name):
            if name[0] == "XH":
                return x_all.at[name[1], name[2], x_rows(core, mid), :]
            return x_all.at[name[1], :, x_rows(core, name[2]), :]

        def x_out(src, there):
            if there[0] == "XH":
                return x_all.at[there[1], there[2], x_rows(core, src[2]), :]
            return x_slot(src)

        def remote(src, dst, ssem, rsem, device):
            copy = pltpu.make_async_remote_copy(src_ref=src, dst_ref=dst, send_sem=ssem, recv_sem=rsem, device_id=device, device_id_type=MESH)
            copy.start()
            sent.append(copy)

        def landed(slot, rsem):
            pltpu.make_async_remote_copy(src_ref=slot, dst_ref=slot, send_sem=l_sem.at[0], recv_sem=rsem, device_id=sibling, device_id_type=MESH).wait_recv()

        def columns(block):
            return pl.ds(pl.multiple_of(block * sub, sub), sub)

        own_a = pltpu.make_async_copy(w_ref, a_all.at[pl.ds(0, rows), pl.ds(0, kcols)], l_sem.at[1])

        def exchange_x(r):
            s = lax.rem(xpos + x_col, 2)
            n = (1 - cross) * RHS + r
            for hops in (1, 3, 2, 0):
                src = x_ref.at[r, :, columns(lax.rem(xpos + hops, XS))]
                dst = x_all.at[n, s, x_rows(core, 0), :]
                ssem, rsem = t_ssem.at[r * XS + hops], t_rsem.at[n * 2 + s]
                if hops == 0:
                    pl.when(cross == 0)(lambda: pltpu.make_async_copy(src, dst, rsem).start())

                    @pl.when(cross == 1)
                    def _():
                        pltpu.make_async_remote_copy(src_ref=src, dst_ref=dst, send_sem=ssem, recv_sem=rsem, device_id=at(0, 3 - col), device_id_type=MESH).start()
                else:
                    remote(src, dst, ssem, rsem, at(hops, x_col))

        def matmul(n, lo, hi):
            kstep = kcols if hi - lo <= 4 else kcols // 2

            def body(idx, carry):
                k0 = pl.multiple_of(idx * kstep, kstep)
                lhs = a_all[pl.ds(lo * hrows, (hi - lo) * hrows), pl.ds(k0, kstep)]
                rhs = x_all[n, idx // (kcols // kstep), pl.ds(pl.multiple_of(lax.rem(k0, kcols), kstep), kstep), :]
                prod = jnp.dot(lhs, rhs, preferred_element_type=jnp.float32)
                acc[n, pl.ds(lo, hi - lo)] += prod.reshape(hi - lo, hrows, sub)
                return carry

            lax.fori_loop(0, 2 * kcols // kstep, body, 0)

        def exchange_acc(n, lo, hi):
            span = pl.ds(lo, hi - lo)
            remote(acc.at[n, span], peer_acc.at[n, span], e_ssem.at[n * BLOCKS + lo], e_rsem.at[n * BLOCKS + lo], links["yp"])

        local = []

        def finish(r, pos):
            dx = next(d for d in POS if POS[d] == pos // 2)
            half = pos % 2
            y_buf[r, pos] = (acc[RHS + r, pos] + peer_acc[r, pos]).astype(y_buf.dtype)
            src, dst = y_buf.at[r, pos], o_ref.at[r, pl.ds(half * hrows, hrows), columns(xpos)]
            sem = (r * XS + dx) * 2 + half
            if dx == 0:
                copy = pltpu.make_async_copy(src, dst, y_ssem.at[sem])
                copy.start()
                local.append(copy)
            else:
                remote(src, dst, y_ssem.at[sem], y_rsem.at[sem], at(XS - dx, col))

        waited = set()
        for step in steps:
            if step[0] == "a2a":
                exchange_x(step[1])
                if step[1] == RHS - 1:
                    own_a.start()
                    acc[...] = jnp.zeros_like(acc)
            elif step[0] == "send":
                _, link, src, dst = step
                if dst[0] == "A":
                    if src[1:3] == (0, 0):
                        ref = w_ref.at[pl.ds(src[3] * hrows + src[4] * unit, unit), :]
                    else:
                        ref = a_slot(src)
                    idx = a_index(dst)
                    remote(ref, a_slot(dst), a_ssem.at[idx], a_rsem.at[idx], links[link])
                else:
                    idx = x_index(dst)
                    ref = x_out(src, dst)
                    remote(ref, ref, x_ssem.at[idx], x_rsem.at[idx], links[link])
            elif step[0] == "wait":
                name = step[1]
                if name[0] == "A":
                    landed(a_slot(name), a_rsem.at[a_index(name)])
                elif name[0] == "T":
                    for s in range(2):
                        landed(x_all.at[name[1], s, x_rows(core, 0), :], t_rsem.at[name[1] * 2 + s])
                else:
                    landed(x_slot(name), x_rsem.at[x_index(name)])
            elif step[0] == "share":
                _, n, dz = step
                slot = x_all.at[n, :, x_rows(core, dz), :]
                remote(slot, slot, d_ssem.at[n * depth_size + dz], d_rsem.at[n * depth_size + dz], sibling)
            elif step[0] == "mm":
                _, n, lo, hi = step
                if "a" not in waited:
                    waited.add("a")
                    own_a.wait()
                if n not in waited:
                    waited.add(n)
                    for dz in range(depth_size):
                        landed(x_all.at[n, :, x_rows(1 - core, dz), :], d_rsem.at[n * depth_size + dz])
                matmul(n, lo, hi)
            elif step[0] == "xch":
                exchange_acc(*step[1:])
            elif step[0] == "peer":
                _, n, lo, hi = step
                landed(peer_acc.at[n, pl.ds(lo, hi - lo)], e_rsem.at[n * BLOCKS + lo])
            else:
                finish(step[1], step[2])

        for r in range(RHS):
            for dx in range(1, XS):
                for half in range(2):
                    slot = o_ref.at[r, pl.ds(half * hrows, hrows), columns(lax.rem(xpos + dx, XS))]
                    landed(slot, y_rsem.at[(r * XS + dx) * 2 + half])

            @pl.when(cross == 1)
            def _():
                src = x_ref.at[r, :, columns(xpos)]
                pltpu.make_async_remote_copy(src_ref=src, dst_ref=src, send_sem=t_ssem.at[r * XS], recv_sem=t_rsem.at[0], device_id=at(0, 3 - col), device_id_type=MESH).wait_send()
        for copy in local:
            copy.wait()
        for copy in sent:
            copy.wait_send()

    def local_product(w_local, x_local):
        rows, kcols = w_local.shape
        sub = x_local.shape[2] // 4
        dma = pltpu.SemaphoreType.DMA

        def sems(size):
            return [dma((size,)), dma((size,))]

        return pl.pallas_call(
            kernel,
            out_shape=jax.ShapeDtypeStruct(x_local.shape, jnp.bfloat16),
            in_specs=[pl.BlockSpec(memory_space=pl.ANY)] * 2,
            out_specs=pl.BlockSpec(memory_space=pl.ANY),
            scratch_shapes=[
                pltpu.VMEM((XS * rows, 2 * kcols), jnp.bfloat16),
                pltpu.VMEM((CHUNKS, 2, kcols, sub), jnp.bfloat16),
                pltpu.VMEM((CHUNKS, BLOCKS, rows // 2, sub), jnp.float32),
                pltpu.VMEM((RHS, BLOCKS, rows // 2, sub), jnp.float32),
                pltpu.VMEM((RHS, BLOCKS, rows // 2, sub), jnp.bfloat16),
                *sems(32), *sems(CHUNKS * (depth_size + 1)), *sems(CHUNKS * depth_size),
                dma((RHS * XS,)), dma((CHUNKS * 2,)), *sems(RHS * BLOCKS), *sems(RHS * BLOCKS), dma((2,)),
            ],
            compiler_params=pltpu.CompilerParams(collective_id=0, has_side_effects=True, vmem_limit_bytes=67043328),
            cost_estimate=pl.CostEstimate(flops=2 * XS * rows * 2 * kcols * CHUNKS * sub, bytes_accessed=0, transcendentals=0),
            name="gather_matmul",
        )(w_local, x_local)

    return jax.shard_map(local_product, mesh=mesh, in_specs=(P(("row", "depth"), "col"), P(None, ("row", "depth"), "col")), out_specs=P(None, ("row", "depth"), "col"), check_vma=False)
```
